16 devices in a mesh: rep: 2 (over y, z), dp: 8 (over x, core).
Axes of the slice: x: 4, y: 2, z: 1, core: 2. Of those that a mesh axis runs over, the one named last changes fastest.
The devices are a block of a 4x4x8 slice.
Arguments:
- g_w_gate: bfloat16 [16, 2, 1024, 2816], P(('rep', 'dp')), parts along dimension 0
- g_w_up: bfloat16 [16, 2, 1024, 2816], P(('rep', 'dp')), parts along dimension 0
- g_w_down: bfloat16 [16, 2, 2816, 1024], P(('rep', 'dp')), parts along dimension 0
- w_gate: bfloat16 [2, 1024, 2816], replicated
- w_up: bfloat16 [2, 1024, 2816], replicated
- w_down: bfloat16 [2, 2816, 1024], replicated
- m_w_gate: float32 [2, 1024, 2816], P(None, 'dp')
- m_w_up: float32 [2, 1024, 2816], P(None, 'dp')
- m_w_down: float32 [2, 2816, 1024], P(None, 'dp')
- v_w_gate: float32 [2, 1024, 2816], P(None, 'dp')
- v_w_up: float32 [2, 1024, 2816], P(None, 'dp')
- v_w_down: float32 [2, 2816, 1024], P(None, 'dp')
Outputs:
- output 1: bfloat16 [4, 1024, 2816], P('rep'), parts along dimension 0
- output 2: bfloat16 [4, 1024, 2816], P('rep'), parts along dimension 0
- output 3: bfloat16 [4, 2816, 1024], P('rep'), parts along dimension 0
- output 4: float32 [4, 1024, 2816], P('rep', 'dp'), parts along dimension 0
- output 5: float32 [4, 1024, 2816], P('rep', 'dp'), parts along dimension 0
- output 6: float32 [4, 2816, 1024], P('rep', 'dp'), parts along dimension 0
- output 7: float32 [4, 1024, 2816], P('rep', 'dp'), parts along dimension 0
- output 8: float32 [4, 1024, 2816], P('rep', 'dp'), parts along dimension 0
- output 9: float32 [4, 2816, 1024], P('rep', 'dp'), parts along dimension 0
There are 2 independent parts. The reference program is written for one: setup_inputs(seed, part) draws one part's arguments, and reference() takes and returns one part's arrays. A program takes and returns all parts, laid end to end along the dimension named above; an argument that names none is the same for every part.
All inputs are finite; a program needn't handle non-finite values.
Results may differ from the reference program's by a relative error of at most 0.022.
Values are sent between devices in bfloat16 or wider.
A program may use at most 768 MiB of HBM per device.

```python
import jax
import jax.numpy as jnp
from jax import lax

DEVICES = 8
D = 1024
FF = 2816
LAYERS = 2
NAMES = ("w_gate", "w_up", "w_down")
SHAPES = {"w_gate": (LAYERS, D, FF), "w_up": (LAYERS, D, FF), "w_down": (LAYERS, FF, D)}


def setup_inputs(seed: int = 0, part: int = 0) -> dict:
    kz, *keys = jax.random.split(jax.random.key(seed), 1 + 5 * len(NAMES))
    loud = 2.0 ** jax.random.uniform(kz, (), jnp.float32, -1.0, 1.0)
    drawn = {}
    for name, key, both in zip(NAMES, keys[:3], keys[3:6], strict=True):
        own = jax.random.normal(jax.random.fold_in(key, part), (DEVICES, *SHAPES[name]), jnp.float32)
        shared = jax.random.normal(jax.random.fold_in(both, part), SHAPES[name], jnp.float32)
        drawn["g_" + name] = (loud * (0.7 * shared / DEVICES + 0.7 * own * DEVICES**-0.5)).astype(jnp.bfloat16)
    for name, key in zip(NAMES, keys[6:9], strict=True):
        drawn[name] = (jax.random.normal(key, SHAPES[name], jnp.float32) * SHAPES[name][1] ** -0.5).astype(jnp.bfloat16)
    for name, key in zip(NAMES, keys[9:12], strict=True):
        drawn["m_" + name] = loud * 0.5 * jax.random.normal(key, SHAPES[name], jnp.float32)
    for name, key in zip(NAMES, keys[12:15], strict=True):
        drawn["v_" + name] = loud * loud * jax.random.uniform(key, SHAPES[name], jnp.float32, 0.5, 1.5)
    return drawn


def adamw(w, m, v, g):
    m = 0.9 * m + 0.1 * g
    v = 0.95 * v + 0.05 * g * g
    step = m * lax.rsqrt(v + 1e-8) + 0.1 * w
    return (w - 0.02 * step).astype(jnp.bfloat16), m, v


def clipped(gradients, sum_of_squares, count):
    factor = jnp.minimum(1.0, 0.5 * lax.rsqrt(sum_of_squares / count + 1e-30))
    return [g * factor for g in gradients]


def reference(g_w_gate, g_w_up, g_w_down, w_gate, w_up, w_down, m_w_gate, m_w_up, m_w_down, v_w_gate, v_w_up, v_w_down):
    def total(terms):
        return lax.scan(lambda so_far, term: (so_far + term.astype(jnp.float32), None), jnp.zeros(terms.shape[1:], jnp.float32), terms)[0]

    gradients = [total(terms).astype(jnp.bfloat16).astype(jnp.float32) for terms in (g_w_gate, g_w_up, g_w_down)]
    gradients = clipped(gradients, sum(jnp.sum(g * g) for g in gradients), sum(g.size for g in gradients))
    new = [
        adamw(w.astype(jnp.float32), m, v, g)
        for w, m, v, g in zip((w_gate, w_up, w_down), (m_w_gate, m_w_up, m_w_down), (v_w_gate, v_w_up, v_w_down), gradients, strict=True)
    ]
    return tuple(one[which] for which in range(3) for one in new)
```

```python
import functools

import jax
import jax.numpy as jnp
from jax import lax
from jax.experimental import pallas as pl
from jax.experimental.pallas import tpu as pltpu
from jax.sharding import PartitionSpec as P

AXIS = "dp"
CORES = 2
AHEAD = 6
GROUP = 16
A, B, C, OWN = 0, 2, 4, 6


def adamw(w, m, v, g):
    m = 0.9 * m + 0.1 * g
    v = 0.95 * v + 0.05 * g * g
    step = m * lax.rsqrt(v + 1e-8) + 0.1 * w
    return (w - 0.02 * step).astype(jnp.bfloat16), m, v


class Places:
    def __init__(self, n, shapes):
        self.n = n
        self.layers = shapes[0][0]
        self.half = [rows // n // 2 for _, rows, _ in shapes]
        self.piece = [(h, cols) for h, (_, _, cols) in zip(self.half, shapes)]
        self.count = len(shapes) * self.layers
        self.kinds = sorted(set(self.piece), key=self.piece.index)
        self.members = [[p for p in range(self.count) if self.piece[p // self.layers] == k] for k in self.kinds]

    def scratch(self, slots, dtype):
        return [pltpu.VMEM((len(m) * slots, *k), dtype) for m, k in zip(self.members, self.kinds)]

    def at(self, buffers, slots, p, slot):
        kind = self.kinds.index(self.piece[p // self.layers])
        return buffers[kind].at[self.members[kind].index(p) * slots + slot]

    def rows(self, refs, p, block, half):
        w = p // self.layers
        start = pl.multiple_of((block * 2 + half) * self.half[w], GROUP)
        return refs[w].at[p % self.layers, pl.ds(start, self.half[w]), :]

    def own(self, refs, p, half):
        w = p // self.layers
        return refs[w].at[p % self.layers, pl.ds(half * self.half[w], self.half[w]), :]


def exchange(places, tail, count, *refs):
    nk = len(places.kinds)
    names = (3, 3, 3, 3, 3, 3, 1, 2 * len(tail), nk, nk, nk, nk, nk, nk, nk, 1, 1, 1, 1, 1, 1, 1, 1, 1)
    parts, i = [], 0
    for size in names:
        parts.append(refs[i : i + size])
        i += size
    g, w, m, v, whole, summed, (factor_ref,), tails = parts[:8]
    own, par, got, mm, vv, ww, acc = parts[8:15]
    (sq,), (own_sem,), (par_send,), (par_recv,), (snd,), (rcv,), (mvw_sem,), (sq_send,), (sq_recv,) = parts[15:]

    n, at = places.n, places.at
    chips = n // CORES
    me = lax.axis_index(AXIS)
    core, chip = lax.rem(me, CORES), lax.div(me, CORES)
    away = lambda k, core: lax.rem(chip + (k + chips), chips) * CORES + core
    partner = away(0, 1 - core)
    sign = (1, -1)
    beside = [away(s, core) for s in sign]

    def remote(src, dst, send, recv, device):
        return pltpu.make_async_remote_copy(
            src_ref=src, dst_ref=dst, send_sem=send, recv_sem=recv, device_id={AXIS: device}, device_id_type=pl.DeviceIdType.MESH
        )

    def place(kind):
        i = kind % 2
        if kind < B:
            return 2, 1 - i, i
        if kind < C:
            return sign[i], i, 2 + i
        if kind < OWN:
            return sign[i], 1 - i, i
        return 0, i, 3 - i

    spots = range(places.count)
    steps = [(k + i, p) for k in (A, B, C) for p in spots for i in range(2)] + [(OWN + h, p) for p in spots for h in (1, 0)]

    def load(kind, p):
        to, half, slot = place(kind)
        return pltpu.make_async_copy(places.rows(g, p, away(to, core), half), at(own, 4, p, slot), own_sem.at[p, slot])

    def give(kind, p):
        to, half, _ = place(kind)
        return remote(places.rows(g, p, away(to, 1 - core), half), at(par, 8, p, kind), par_send.at[p, kind], par_recv.at[p, kind], partner)

    def send(kind, p):
        slot = place(kind)[2]
        return remote(at(own, 4, p, slot), at(got, 6, p, kind), snd.at[p, kind], rcv.at[p, kind], beside[kind % 2])

    def start_load(t):
        kind, p = steps[t]
        if kind >= C:
            send(kind - C if kind < OWN else B + 1 - (kind - OWN), p).wait_send()
        load(kind, p).start()

    def add_up(kind, p):
        out = at(own, 4, p, place(kind)[2])
        terms = [out, at(par, 8, p, kind)]
        if C <= kind < OWN:
            terms.append(at(got, 6, p, kind - C))
        if kind >= OWN:
            i = 1 - (kind - OWN)
            terms += [at(got, 6, p, C + i), at(got, 6, p, B + 1 - i)]
        squares = acc[places.kinds.index(places.piece[p // places.layers])]

        def body(r, carry):
            rows = pl.ds(pl.multiple_of(r * GROUP, GROUP), GROUP)
            total = terms[0][rows, :].astype(jnp.float32)
            for one in terms[1:]:
                total = total + one[rows, :].astype(jnp.float32)
            total = total.astype(jnp.bfloat16)
            out[rows, :] = total
            if kind >= OWN:
                total = total.astype(jnp.float32)
                squares[...] += total * total
            return carry

        lax.fori_loop(0, places.half[p // places.layers] // GROUP, body, 0)

    def moments(p, h):
        return [
            pltpu.make_async_copy(places.own(m, p, h), at(mm, 2, p, h), mvw_sem.at[p, h, 0]),
            pltpu.make_async_copy(places.own(v, p, h), at(vv, 2, p, h), mvw_sem.at[p, h, 1]),
            pltpu.make_async_copy(places.rows(w, p, me, h), at(ww, 2, p, h), mvw_sem.at[p, h, 2]),
        ]

    for t in range(AHEAD):
        start_load(t)
    barrier = pltpu.get_barrier_semaphore()
    for o in range(1, n):
        pl.semaphore_signal(barrier, inc=1, device_id={AXIS: lax.rem(me + o, n)}, device_id_type=pl.DeviceIdType.MESH)
    pl.semaphore_wait(barrier, n - 1)
    for t in range(AHEAD):
        give(*steps[t]).start()
    for one in acc:
        one[...] = jnp.zeros_like(one)

    for t, (kind, p) in enumerate(steps):
        if t + AHEAD < len(steps):
            give(*steps[t + AHEAD]).start()
        load(kind, p).wait()
        give(kind, p).wait_recv()
        if C <= kind < OWN:
            send(kind - C, p).wait_recv()
        if kind >= OWN:
            i = 1 - (kind - OWN)
            send(B + 1 - i, p).wait_recv()
            send(C + i, p).wait_recv()
        add_up(kind, p)
        if kind < OWN:
            send(kind, p).start()
        if t + AHEAD < len(steps):
            start_load(t + AHEAD)
        if t == 2 * places.count:
            for q in spots:
                for h in range(2):
                    for copy in moments(q, h):
                        copy.start()

    sq[me] = jnp.full(sq.shape[1:], sum(jnp.sum(one[...]) for one in acc), jnp.float32)

    def tell(o, device):
        return remote(sq.at[device], sq.at[device], sq_send.at[o], sq_recv.at[o], lax.rem(me + o, n))

    for o in range(1, n):
        tell(o, me).start()
    for p in spots:
        for i in range(2):
            send(C + i, p).wait_send()
        for kind in range(8):
            give(kind, p).wait_send()
    for o in range(1, n):
        tell(o, lax.rem(me + (n - o), n)).wait_recv()
    for o in range(1, n):
        tell(o, me).wait_send()
    total = sq[0]
    for d in range(1, n):
        total = total + sq[d]
    factor_ref[...] = jnp.minimum(1.0, 0.5 * lax.rsqrt(total / count + 1e-30))

    def ahead(i, p, h):
        k = 2 * i + h
        return remote(at(ww, 2, p, h), places.rows(whole, p, me, h), snd.at[p, k], rcv.at[p, k], beside[i])

    def ahead_came(i, p, h):
        k = 2 * i + h
        here = places.rows(whole, p, away(-sign[i], core), h)
        return remote(here, here, snd.at[p, k], rcv.at[p, k], beside[i])

    def onward(i, p):
        here = places.rows(whole, p, away(-sign[i], core), 1 - i)
        return remote(here, here, snd.at[p, 4 + i], rcv.at[p, 4 + i], beside[i])

    def onward_came(i, p):
        here = places.rows(whole, p, away(2, core), 1 - i)
        return remote(here, here, snd.at[p, 4 + i], rcv.at[p, 4 + i], beside[i])

    def across(k, p):
        if k < 4:
            here = places.rows(whole, p, away(-sign[k // 2], core), k % 2)
        elif k < 6:
            here = places.rows(whole, p, away(2, core), 1 - (k - 4))
        else:
            here = places.rows(whole, p, me, k - 6)
        src = here if k < 6 else at(ww, 2, p, k - 6)
        return remote(src, here, par_send.at[p, k], par_recv.at[p, k], partner)

    def across_came(k, p):
        if k < 4:
            here = places.rows(whole, p, away(-sign[k // 2], 1 - core), k % 2)
        elif k < 6:
            here = places.rows(whole, p, away(2, 1 - core), 1 - (k - 4))
        else:
            here = places.rows(whole, p, partner, k - 6)
        return remote(here, here, par_send.at[p, k], par_recv.at[p, k], partner)

    def keep(p, h):
        return [
            pltpu.make_async_copy(at(ww, 2, p, h), places.rows(whole, p, me, h), own_sem.at[p, h]),
            pltpu.make_async_copy(at(own, 4, p, 3 - h), places.own(summed, p, h), own_sem.at[p, 2 + h]),
        ]

    def hand(p, h):
        return pltpu.make_async_copy(at(ww, 2, p, h), tails[2 * tail.index(p) + h], mvw_sem.at[p, h, 0])

    def update(p, h):
        for copy in moments(p, h):
            copy.wait()
        gs, ms, vs, ws = at(own, 4, p, 3 - h), at(mm, 2, p, h), at(vv, 2, p, h), at(ww, 2, p, h)

        def body(r, carry):
            rows = pl.ds(pl.multiple_of(r * GROUP, GROUP), GROUP)
            grad = gs[rows, :].astype(jnp.float32) * factor_ref[0:1, 0:1]
            ws[rows, :] = adamw(ws[rows, :].astype(jnp.float32), ms[rows, :], vs[rows, :], grad)[0]
            return carry

        lax.fori_loop(0, places.half[p // places.layers] // GROUP, body, 0)

    for p in spots:
        for h in (1, 0):
            update(p, h)
            ahead(1 - h, p, h).start()
            across(6 + h, p).start()
            for copy in keep(p, h):
                copy.start()
            if p in tail:
                hand(p, h).start()
    later = [p for p in spots if p not in tail]
    for p in later:
        for h in (0, 1):
            ahead(h, p, h).start()
    for p in spots:
        for i in range(2):
            ahead_came(i, p, 1 - i).wait_recv()
            onward(i, p).start()
            across(2 * i + 1 - i, p).start()
    for p in later:
        for i in range(2):
            ahead_came(i, p, i).wait_recv()
            across(2 * i + i, p).start()
    for p in spots:
        for i in range(2):
            onward_came(i, p).wait_recv()
            across(4 + i, p).start()
    for p in spots:
        for h in range(2):
            ahead(1 - h, p, h).wait_send()
            if p in later:
                ahead(h, p, h).wait_send()
            onward(h, p).wait_send()
            for copy in keep(p, h):
                copy.wait()
            if p in tail:
                hand(p, h).wait()
        for k in range(8):
            if k in (0, 3) and p in tail:
                continue
            across(k, p).wait_send()
            across_came(k, p).wait_recv()


def gather_new(terms, weights, m, v, n, tail):
    shapes = [w.shape for w in weights]
    places = Places(n, shapes)
    count = float(sum(w.size for w in weights))
    anywhere, vmem = pl.BlockSpec(memory_space=pl.ANY), pl.BlockSpec(memory_space=pltpu.VMEM)
    out = [jax.ShapeDtypeStruct(s, jnp.bfloat16) for s in shapes]
    out += [jax.ShapeDtypeStruct(one.shape, jnp.bfloat16) for one in m]
    out += [jax.ShapeDtypeStruct((8, 128), jnp.float32)]
    out += [jax.ShapeDtypeStruct(places.piece[p // places.layers], jnp.bfloat16) for p in tail for _ in range(2)]
    dma = pltpu.SemaphoreType.DMA
    half = jnp.bfloat16
    scratch = [
        *places.scratch(4, half), *places.scratch(8, half), *places.scratch(6, half),
        *places.scratch(2, jnp.float32), *places.scratch(2, jnp.float32), *places.scratch(2, half),
        *(pltpu.VMEM((GROUP, k[1]), jnp.float32) for k in places.kinds),
        pltpu.VMEM((n, 8, 128), jnp.float32),
        dma((places.count, 4)), dma((places.count, 8)), dma((places.count, 8)), dma((places.count, 6)), dma((places.count, 6)),
        dma((places.count, 2, 3)), dma((n,)), dma((n,)),
    ]
    got = pl.pallas_call(
        functools.partial(exchange, places, tail, count),
        out_shape=out,
        in_specs=[anywhere] * 12,
        out_specs=[anywhere] * 6 + [vmem] + [anywhere] * (2 * len(tail)),
        scratch_shapes=scratch,
        compiler_params=pltpu.CompilerParams(collective_id=0, has_side_effects=True, vmem_limit_bytes=66 * 1000 * 1000),
        name="exchange",
    )(*terms, *weights, *m, *v)
    return got[:3], got[3:6], got[6], got[7:]


def solution(mesh):
    n = mesh.shape[AXIS]

    def step(*arrays):
        terms, weights, m, v = (arrays[i : i + 3] for i in (0, 3, 6, 9))
        whole, summed, factor, _ = gather_new([t[0] for t in terms], weights, m, v, n, [])
        grads = [g.astype(jnp.float32) * factor[0, 0] for g in summed]
        new_m = [0.9 * a + 0.1 * g for a, g in zip(m, grads)]
        new_v = [0.95 * a + 0.05 * g * g for a, g in zip(v, grads)]
        return (*whole, *new_m, *new_v)

    all_of, cut = P(None, None, None), P(None, AXIS, None)
    return jax.shard_map(
        step,
        mesh=mesh,
        in_specs=(P(("rep", AXIS), None, None, None),) * 3 + (all_of,) * 3 + (cut,) * 6,
        out_specs=(P("rep", None, None),) * 3 + (P("rep", AXIS, None),) * 6,
        check_vma=False,
    )
```

```python
import functools

import jax
import jax.numpy as jnp
from jax import lax
from jax.experimental import pallas as pl
from jax.experimental.pallas import tpu as pltpu
from jax.sharding import PartitionSpec as P


AXIS = "dp"
CORES = 2
AHEAD = 6
GROUP = 16
FIRST = 2
SLOTS, DEPTH = 24, 12
A, B, C, OWN = 0, 2, 4, 6


def adamw(w, m, v, g):
    m = 0.9 * m + 0.1 * g
    v = 0.95 * v + 0.05 * g * g
    step = m * lax.rsqrt(v + 1e-8) + 0.1 * w
    return (w - 0.02 * step).astype(jnp.bfloat16), m, v


class Places:
    def __init__(self, n, shapes):
        self.n = n
        self.layers = shapes[0][0]
        self.half = [rows // n // 2 for _, rows, _ in shapes]
        self.piece = [(h, cols) for h, (_, _, cols) in zip(self.half, shapes)]
        self.count = len(shapes) * self.layers
        self.kinds = sorted(set(self.piece), key=self.piece.index)
        self.members = [[p for p in range(self.count) if self.piece[p // self.layers] == k] for k in self.kinds]

    def scratch(self, slots, dtype):
        return [pltpu.VMEM((len(m) * slots, *k), dtype) for m, k in zip(self.members, self.kinds)]

    def spot(self, p):
        kind = self.kinds.index(self.piece[p // self.layers])
        return kind, self.members[kind].index(p)

    def at(self, buffers, slots, p, slot):
        kind, j = self.spot(p)
        return buffers[kind].at[j * slots + slot]

    def rows(self, refs, p, block, half):
        w = p // self.layers
        start = pl.multiple_of((block * 2 + half) * self.half[w], GROUP)
        return refs[w].at[p % self.layers, pl.ds(start, self.half[w]), :]

    def own(self, refs, p, half):
        w = p // self.layers
        return refs[w].at[p % self.layers, pl.ds(half * self.half[w], self.half[w]), :]


def exchange(places, tail, count, *refs):
    nk = len(places.kinds)
    names = (3, 3, 3, 3, 3, 3, 1, 2 * nk + 1, nk, nk, nk, nk, nk, nk, nk, 1, 1, 1, 1, 1, 1, 1, 1, 1)
    parts, i = [], 0
    for size in names:
        parts.append(refs[i : i + size])
        i += size
    g, w, m, v, whole, summed, (factor_ref,), (*tails, last) = parts[:8]
    own, par, got, mm, vv, ww, acc = parts[8:15]
    (sq,), (own_sem,), (par_send,), (par_recv,), (snd,), (rcv,), (mvw_sem,), (sq_send,), (sq_recv,) = parts[15:]

    n, at = places.n, places.at
    chips = n // CORES
    me = lax.axis_index(AXIS)
    core, chip = lax.rem(me, CORES), lax.div(me, CORES)
    away = lambda k, core: lax.rem(chip + (k + chips), chips) * CORES + core
    partner = away(0, 1 - core)
    sign = (1, -1)
    beside = [away(s, core) for s in sign]

    def remote(src, dst, send, recv, device):
        return pltpu.make_async_remote_copy(
            src_ref=src, dst_ref=dst, send_sem=send, recv_sem=recv, device_id={AXIS: device}, device_id_type=pl.DeviceIdType.MESH
        )

    def place(kind):
        i = kind % 2
        if kind < B:
            return 2, 1 - i, i
        if kind < C:
            return sign[i], i, 2 + i
        if kind < OWN:
            return sign[i], 1 - i, i
        return 0, i, 3 - i

    spots = range(places.count)
    steps = [(k + i, p) for k in (A, B, C) for p in spots for i in range(2)] + [(OWN + h, p) for p in spots for h in (1, 0)]

    def load(kind, p):
        to, half, slot = place(kind)
        return pltpu.make_async_copy(places.rows(g, p, away(to, core), half), at(own, 4, p, slot), own_sem.at[p, slot])

    def give(kind, p):
        to, half, _ = place(kind)
        return remote(places.rows(g, p, away(to, 1 - core), half), at(par, 8, p, kind), par_send.at[p, kind], par_recv.at[p, kind], partner)

    def send(kind, p):
        slot = place(kind)[2]
        return remote(at(own, 4, p, slot), at(got, 6, p, kind), snd.at[p, kind], rcv.at[p, kind], beside[kind % 2])

    def start_load(t):
        kind, p = steps[t]
        if kind >= C:
            send(kind - C if kind < OWN else B + 1 - (kind - OWN), p).wait_send()
        load(kind, p).start()

    def add_up(kind, p):
        out = at(own, 4, p, place(kind)[2])
        terms = [out, at(par, 8, p, kind)]
        if C <= kind < OWN:
            terms.append(at(got, 6, p, kind - C))
        if kind >= OWN:
            i = 1 - (kind - OWN)
            terms += [at(got, 6, p, C + i), at(got, 6, p, B + 1 - i)]
        squares = acc[places.kinds.index(places.piece[p // places.layers])]

        def body(r, carry):
            rows = pl.ds(pl.multiple_of(r * GROUP, GROUP), GROUP)
            total = terms[0][rows, :].astype(jnp.float32)
            for one in terms[1:]:
                total = total + one[rows, :].astype(jnp.float32)
            total = total.astype(jnp.bfloat16)
            out[rows, :] = total
            if kind >= OWN:
                total = total.astype(jnp.float32)
                squares[...] += total * total
            return carry

        lax.fori_loop(0, places.half[p // places.layers] // GROUP, body, 0)

    def moments(p, h):
        return [
            pltpu.make_async_copy(places.own(m, p, h), at(mm, 2, p, h), mvw_sem.at[p, h, 0]),
            pltpu.make_async_copy(places.own(v, p, h), at(vv, 2, p, h), mvw_sem.at[p, h, 1]),
            pltpu.make_async_copy(places.rows(w, p, me, h), at(ww, 2, p, h), mvw_sem.at[p, h, 2]),
        ]

    for t in range(AHEAD):
        start_load(t)
    barrier = pltpu.get_barrier_semaphore()
    for device in (partner, *beside):
        pl.semaphore_signal(barrier, inc=1, device_id={AXIS: device}, device_id_type=pl.DeviceIdType.MESH)
    pl.semaphore_wait(barrier, 3)
    for t in range(FIRST):
        give(*steps[t]).start()
    for one in acc:
        one[...] = jnp.zeros_like(one)

    given = lambda t: min(FIRST + 2 * t, t + AHEAD, len(steps))
    for t, (kind, p) in enumerate(steps):
        load(kind, p).wait()
        give(kind, p).wait_recv()
        for ahead in range(given(t), given(t + 1)):
            give(*steps[ahead]).start()
        if C <= kind < OWN:
            send(kind - C, p).wait_recv()
        if kind >= OWN:
            i = 1 - (kind - OWN)
            send(B + 1 - i, p).wait_recv()
            send(C + i, p).wait_recv()
        add_up(kind, p)
        if kind < OWN:
            send(kind, p).start()
        if t + AHEAD < len(steps):
            start_load(t + AHEAD)
        if t == 2 * places.count:
            for q in spots:
                for h in range(2):
                    for copy in moments(q, h):
                        copy.start()

    sq[me] = jnp.full(sq.shape[1:], sum(jnp.sum(one[...]) for one in acc), jnp.float32)

    def tell(o, device):
        return remote(sq.at[device], sq.at[device], sq_send.at[o], sq_recv.at[o], lax.rem(me + o, n))

    for o in range(1, n):
        tell(o, me).start()
    for p in spots:
        for i in range(2):
            send(C + i, p).wait_send()
        for kind in range(8):
            give(kind, p).wait_send()
    for o in range(1, n):
        tell(o, lax.rem(me + (n - o), n)).wait_recv()
    for o in range(1, n):
        tell(o, me).wait_send()
    total = sq[0]
    for d in range(1, n):
        total = total + sq[d]
    factor_ref[...] = jnp.minimum(1.0, 0.5 * lax.rsqrt(total / count + 1e-30))

    def ahead(i, p, h):
        k = 2 * i + h
        return remote(at(ww, 2, p, h), places.rows(whole, p, me, h), snd.at[p, k], rcv.at[p, k], beside[i])

    def ahead_came(i, p, h):
        k = 2 * i + h
        here = places.rows(whole, p, away(-sign[i], core), h)
        return remote(here, here, snd.at[p, k], rcv.at[p, k], beside[i])

    def onward(i, p):
        here = places.rows(whole, p, away(-sign[i], core), 1 - i)
        there = last.at[i] if p == places.count - 1 else here
        return remote(here, there, snd.at[p, 4 + i], rcv.at[p, 4 + i], beside[i])

    def onward_came(i, p):
        here = last.at[i] if p == places.count - 1 else places.rows(whole, p, away(2, core), 1 - i)
        return remote(here, here, snd.at[p, 4 + i], rcv.at[p, 4 + i], beside[i])

    def across(k, p):
        if k < 4:
            here = places.rows(whole, p, away(-sign[k // 2], core), k % 2)
        elif k < 6:
            here = places.rows(whole, p, away(2, core), 1 - (k - 4))
        else:
            here = places.rows(whole, p, me, k - 6)
        src = here if k < 6 else at(ww, 2, p, k - 6)
        return remote(src, here, par_send.at[p, k], par_recv.at[p, k], partner)

    def across_came(k, p):
        if k < 4:
            here = places.rows(whole, p, away(-sign[k // 2], 1 - core), k % 2)
        elif k < 6:
            here = places.rows(whole, p, away(2, 1 - core), 1 - (k - 4))
        else:
            here = places.rows(whole, p, partner, k - 6)
        return remote(here, here, par_send.at[p, k], par_recv.at[p, k], partner)

    def keep(p, h):
        return [
            pltpu.make_async_copy(at(ww, 2, p, h), places.rows(whole, p, me, h), own_sem.at[p, h]),
            pltpu.make_async_copy(at(own, 4, p, 3 - h), places.own(summed, p, h), own_sem.at[p, 2 + h]),
        ]

    def hand(p, h):
        kind, j = places.spot(p)
        return pltpu.make_async_copy(at(ww, 2, p, h), tails[2 * kind + h].at[j], mvw_sem.at[p, h, 0])

    def update(p, h):
        for copy in moments(p, h):
            copy.wait()
        gs, ms, vs, ws = at(own, 4, p, 3 - h), at(mm, 2, p, h), at(vv, 2, p, h), at(ww, 2, p, h)

        def body(r, carry):
            rows = pl.ds(pl.multiple_of(r * GROUP, GROUP), GROUP)
            grad = gs[rows, :].astype(jnp.float32) * factor_ref[0:1, 0:1]
            ws[rows, :] = adamw(ws[rows, :].astype(jnp.float32), ms[rows, :], vs[rows, :], grad)[0]
            return carry

        lax.fori_loop(0, places.half[p // places.layers] // GROUP, body, 0)

    for p in spots:
        for h in (1, 0):
            update(p, h)
            ahead(1 - h, p, h).start()
            across(6 + h, p).start()
            for copy in keep(p, h):
                copy.start()
            if p in tail:
                hand(p, h).start()
    later = [p for p in spots if p not in tail]
    for p in later:
        for h in (0, 1):
            ahead(h, p, h).start()
    for p in spots:
        for i in range(2):
            ahead_came(i, p, 1 - i).wait_recv()
            onward(i, p).start()
            across(2 * i + 1 - i, p).start()
    for p in later:
        for i in range(2):
            ahead_came(i, p, i).wait_recv()
            across(2 * i + i, p).start()
    for p in spots:
        for i in range(2):
            onward_came(i, p).wait_recv()
            if p < places.count - 1:
                across(4 + i, p).start()
    for p in spots:
        for h in range(2):
            ahead(1 - h, p, h).wait_send()
            if p in later:
                ahead(h, p, h).wait_send()
            onward(h, p).wait_send()
            for copy in keep(p, h):
                copy.wait()
            if p in tail:
                hand(p, h).wait()
        for k in range(8):
            if k in (0, 3) and p in tail or k in (4, 5) and p == places.count - 1:
                continue
            across(k, p).wait_send()
            across_came(k, p).wait_recv()


def gather_new(terms, weights, m, v, n, tail):
    shapes = [w.shape for w in weights]
    places = Places(n, shapes)
    count = float(sum(w.size for w in weights))
    anywhere, vmem = pl.BlockSpec(memory_space=pl.ANY), pl.BlockSpec(memory_space=pltpu.VMEM)
    out = [jax.ShapeDtypeStruct(s, jnp.bfloat16) for s in shapes]
    out += [jax.ShapeDtypeStruct(one.shape, jnp.bfloat16) for one in m]
    out += [jax.ShapeDtypeStruct((8, 128), jnp.float32)]
    out += [jax.ShapeDtypeStruct((len(m), *k), jnp.bfloat16) for m, k in zip(places.members, places.kinds) for _ in range(2)]
    out += [jax.ShapeDtypeStruct((2, *places.piece[-1]), jnp.bfloat16)]
    dma = pltpu.SemaphoreType.DMA
    half = jnp.bfloat16
    scratch = [
        *places.scratch(4, half), *places.scratch(8, half), *places.scratch(6, half),
        *places.scratch(2, jnp.float32), *places.scratch(2, jnp.float32), *places.scratch(2, half),
        *(pltpu.VMEM((GROUP, k[1]), jnp.float32) for k in places.kinds),
        pltpu.VMEM((n, 8, 128), jnp.float32),
        dma((places.count, 4)), dma((places.count, 8)), dma((places.count, 8)), dma((places.count, 6)), dma((places.count, 6)),
        dma((places.count, 2, 3)), dma((n,)), dma((n,)),
    ]
    got = pl.pallas_call(
        functools.partial(exchange, places, tail, count),
        out_shape=out,
        in_specs=[anywhere] * 12,
        out_specs=[anywhere] * 6 + [vmem] + [anywhere] * (2 * len(places.kinds) + 1),
        scratch_shapes=scratch,
        compiler_params=pltpu.CompilerParams(collective_id=0, has_side_effects=True, vmem_limit_bytes=66 * 1000 * 1000),
        name="exchange",
    )(*terms, *weights, *m, *v)
    return got[:3], got[3:6], got[6], got[7:-1], got[-1]


def params(**more):
    return pltpu.CompilerParams(has_side_effects=False, **more)


def finish(places, tail, *refs):
    nk = len(places.kinds)
    parts, i = [], 0
    for size in (3, 3, 3, 3, 1, 3, 3, 3, nk, nk, nk, nk, 1, 1, 1, 1):
        parts.append(refs[i : i + size])
        i += size
    whole, summed, m, v, (factor_ref,), out, new_m, new_v, slots, gg, mm, vv, (in_sem,), (out_sem,), (get_sem,), (put_sem,) = parts
    n = places.n
    chips = n // CORES
    chip = lax.div(lax.axis_index(AXIS), CORES)
    at = places.at

    def gets(p, h):
        refs = ((summed, gg), (m, mm), (v, vv))
        return [pltpu.make_async_copy(places.own(a, p, h), at(b, 2, p, h), get_sem.at[p, h, j]) for j, (a, b) in enumerate(refs)]

    def puts(p, h):
        refs = ((mm, new_m), (vv, new_v))
        return [pltpu.make_async_copy(at(a, 2, p, h), places.own(b, p, h), put_sem.at[p, h, j]) for j, (a, b) in enumerate(refs)]

    pieces = [(p, h) for p in range(places.count) for h in range(2)]
    items = []
    for p, h in pieces:
        for k in range(chips):
            if p in tail and k == (1 if h else chips - 1) or p == places.count - 1 and k == 2:
                continue
            items += [(p, h, k, c) for c in range(CORES)]
    used = [0] * nk
    turn = []
    for p, *_ in items:
        kind = places.kinds.index(places.piece[p // places.layers])
        turn.append((kind, used[kind]))
        used[kind] += 1
    of_kind = [[t for t, (k, _) in enumerate(turn) if k == kind] for kind in range(nk)]

    def ends(t):
        p, h, k, c = items[t]
        block = lax.rem(chip + k, chips) * CORES + c
        kind, u = turn[t]
        return places.rows(whole, p, block, h), slots[kind].at[u % SLOTS], places.rows(out, p, block, h), (kind, u % SLOTS)

    def read(t):
        src, slot, _, sem = ends(t)
        return pltpu.make_async_copy(src, slot, in_sem.at[sem])

    def write(t):
        _, slot, dst, sem = ends(t)
        return pltpu.make_async_copy(slot, dst, out_sem.at[sem])

    def start_read(t):
        kind, u = turn[t]
        if u >= SLOTS:
            write(of_kind[kind][u - SLOTS]).wait()
        read(t).start()

    def update(p, h):
        for copy in gets(p, h):
            copy.wait()
        gs, ms, vs = at(gg, 2, p, h), at(mm, 2, p, h), at(vv, 2, p, h)

        def body(r, carry):
            rows = pl.ds(pl.multiple_of(r * GROUP, GROUP), GROUP)
            grad = gs[rows, :].astype(jnp.float32) * factor_ref[0:1, 0:1]
            ms[rows, :] = 0.9 * ms[rows, :] + 0.1 * grad
            vs[rows, :] = 0.95 * vs[rows, :] + 0.05 * grad * grad
            return carry

        lax.fori_loop(0, places.half[p // places.layers] // GROUP, body, 0)
        for copy in puts(p, h):
            copy.start()

    for t in range(min(DEPTH, len(items))):
        start_read(t)
    for copy in gets(*pieces[0]):
        copy.start()
    done = 0
    for t in range(len(items)):
        read(t).wait()
        write(t).start()
        if t + DEPTH < len(items):
            start_read(t + DEPTH)
        while done < len(pieces) and (done + 1) * len(items) <= (t + 1) * len(pieces):
            if done + 1 < len(pieces):
                for copy in gets(*pieces[done + 1]):
                    copy.start()
            update(*pieces[done])
            done += 1
    for kind in range(nk):
        for t in of_kind[kind][-SLOTS:]:
            write(t).wait()
    for p, h in pieces:
        for copy in puts(p, h):
            copy.wait()


def finish_all(places, tail, whole, summed, m, v, factor):
    anywhere, vmem = pl.BlockSpec(memory_space=pl.ANY), pl.BlockSpec(memory_space=pltpu.VMEM)
    dma = pltpu.SemaphoreType.DMA
    nk, f32 = len(places.kinds), jnp.float32
    size = sum(w.size for w in whole)
    mine = sum(one.size for one in m)
    return pl.pallas_call(
        functools.partial(finish, places, tail),
        out_shape=[jax.ShapeDtypeStruct(w.shape, w.dtype) for w in whole] + [jax.ShapeDtypeStruct(one.shape, f32) for one in (*m, *v)],
        in_specs=[anywhere] * 12 + [vmem],
        out_specs=[anywhere] * 9,
        scratch_shapes=[
            *(pltpu.VMEM((SLOTS, *k), jnp.bfloat16) for k in places.kinds),
            *places.scratch(2, jnp.bfloat16), *places.scratch(2, f32), *places.scratch(2, f32),
            dma((nk, SLOTS)), dma((nk, SLOTS)), dma((places.count, 2, 3)), dma((places.count, 2, 2)),
        ],
        compiler_params=params(vmem_limit_bytes=58 * 1024 * 1024),
        cost_estimate=pl.CostEstimate(flops=size * 100, bytes_accessed=size * 4 + mine * 18, transcendentals=0),
        name="finish",
    )(*whole, *summed, *m, *v, factor)


def place_late(places, spots, *refs):
    k = len(spots)
    arrays, out, sem = refs[:k], refs[k + 3 : k + 6], refs[k + 6]
    chips = places.n // CORES
    me = lax.axis_index(AXIS)
    core, chip = lax.rem(me, CORES), lax.div(me, CORES)
    copies = []
    for array, pieces in zip(arrays, spots):
        for j, (p, h, away, other) in enumerate(pieces):
            block = lax.rem(chip + (away + chips), chips) * CORES + (1 - core if other else core)
            copies.append(pltpu.make_async_copy(array.at[j], places.rows(out, p, block, h), sem.at[len(copies)]))
    for copy in copies:
        copy.start()
    for copy in copies:
        copy.wait()


def place_all(places, spots, arrays, out):
    anywhere, vmem = pl.BlockSpec(memory_space=pl.ANY), pl.BlockSpec(memory_space=pltpu.VMEM)
    k = len(spots)
    return pl.pallas_call(
        functools.partial(place_late, places, spots),
        out_shape=[jax.ShapeDtypeStruct(w.shape, w.dtype) for w in out],
        in_specs=[vmem] * k + [anywhere] * 3,
        out_specs=[anywhere] * 3,
        input_output_aliases={k + j: j for j in range(3)},
        scratch_shapes=[pltpu.SemaphoreType.DMA((sum(len(one) for one in spots),))],
        compiler_params=params(vmem_limit_bytes=16 * 1024 * 1024),
        cost_estimate=pl.CostEstimate(flops=10**7, bytes_accessed=sum(x.size for x in arrays) * 4, transcendentals=0),
        name="place_late",
    )(*arrays, *out)


def solution(mesh):
    n = mesh.shape[AXIS]
    chips = n // CORES

    def step(*arrays):
        terms, weights, m, v = (arrays[i : i + 3] for i in (0, 3, 6, 9))
        places = Places(n, [w.shape for w in weights])
        tail = list(range(places.count))
        whole, summed, factor, late, last = gather_new([t[0] for t in terms], weights, m, v, n, tail)
        kinds = range(len(places.kinds))
        shift = [[(j, (j // CORES + s) % chips * CORES + j % CORES) for j in range(n)] for s in (1, -1)]
        swap = [(j, j // CORES * CORES + (CORES - 1 - j % CORES)) for j in range(n)]
        came = []
        for k in kinds:
            came.append([lax.ppermute(late[2 * k + h], AXIS, shift[h]) for h in range(2)])
        last_swapped = lax.ppermute(last, AXIS, swap)
        *out, m0, m1, m2, v0, v1, v2 = finish_all(places, tail, whole, summed, m, v, factor)
        end = places.count - 1
        spots = lambda k, other: [[(p, h, -1 if h == 0 else 1, other) for p in places.members[k]] for h in range(2)]
        ends = lambda other: [(end, 1 - i, 2, other) for i in range(2)]
        for k in kinds:
            here, out = lax.optimization_barrier((came[k], out))
            swapped = [lax.ppermute(piece, AXIS, swap) for piece in here]
            if k == 0:
                out = place_all(places, [*spots(k, False), ends(False), ends(True)], [*here, last, last_swapped], out)
            else:
                out = place_all(places, spots(k, False), here, out)
            out = place_all(places, spots(k, True), swapped, out)
        return (*out, m0, m1, m2, v0, v1, v2)

    all_of, cut = P(None, None, None), P(None, AXIS, None)
    return jax.shard_map(
        step,
        mesh=mesh,
        in_specs=(P(("rep", AXIS), None, None, None),) * 3 + (all_of,) * 3 + (cut,) * 6,
        out_specs=(P("rep", None, None),) * 3 + (P("rep", AXIS, None),) * 6,
        check_vma=False,
    )
```

```python
import functools

import jax
import jax.numpy as jnp
from jax import lax
from jax.experimental import pallas as pl
from jax.experimental.pallas import tpu as pltpu
from jax.sharding import PartitionSpec as P


AXIS = "dp"
CORES = 2
AHEAD = 6
GROUP = 16
FIRST = 2
SLOTS, DEPTH = 24, 12
A, B, C, OWN = 0, 2, 4, 6


def adamw(w, m, v, g):
    m = 0.9 * m + 0.1 * g
    v = 0.95 * v + 0.05 * g * g
    step = m * lax.rsqrt(v + 1e-8) + 0.1 * w
    return (w - 0.02 * step).astype(jnp.bfloat16), m, v


class Places:
    def __init__(self, n, shapes):
        self.n = n
        self.layers = shapes[0][0]
        self.half = [rows // n // 2 for _, rows, _ in shapes]
        self.piece = [(h, cols) for h, (_, _, cols) in zip(self.half, shapes)]
        self.count = len(shapes) * self.layers
        self.kinds = sorted(set(self.piece), key=self.piece.index)
        self.members = [[p for p in range(self.count) if self.piece[p // self.layers] == k] for k in self.kinds]

        self.end = self.count - 1

    def scratch(self, slots, dtype):
        return [pltpu.VMEM((len(m) * slots, *k), dtype) for m, k in zip(self.members, self.kinds)]

    def spot(self, p):
        kind = self.kinds.index(self.piece[p // self.layers])
        return kind, self.members[kind].index(p)

    def at(self, buffers, slots, p, slot):
        kind, j = self.spot(p)
        return buffers[kind].at[j * slots + slot]

    def rows(self, refs, p, block, half):
        w = p // self.layers
        start = pl.multiple_of((block * 2 + half) * self.half[w], GROUP)
        return refs[w].at[p % self.layers, pl.ds(start, self.half[w]), :]

    def own(self, refs, p, half):
        w = p // self.layers
        return refs[w].at[p % self.layers, pl.ds(half * self.half[w], self.half[w]), :]


def exchange(places, tail, count, *refs):
    nk = len(places.kinds)
    names = (3, 3, 3, 3, 3, nk, nk, 1, 2 * nk + 1, nk, nk, nk, nk, nk, 1, 1, 1, 1, 1, 1, 1, 1, 1)
    parts, i = [], 0
    for size in names:
        parts.append(refs[i : i + size])
        i += size
    g, w, m, v, whole, mm, vv, (factor_ref,), (*tails, last) = parts[:9]
    own, par, got, ww, acc = parts[9:14]
    (sq,), (own_sem,), (par_send,), (par_recv,), (snd,), (rcv,), (mvw_sem,), (sq_send,), (sq_recv,) = parts[14:]

    n, at = places.n, places.at
    chips = n // CORES
    me = lax.axis_index(AXIS)
    core, chip = lax.rem(me, CORES), lax.div(me, CORES)
    away = lambda k, core: lax.rem(chip + (k + chips), chips) * CORES + core
    partner = away(0, 1 - core)
    sign = (1, -1)
    beside = [away(s, core) for s in sign]

    def remote(src, dst, send, recv, device):
        return pltpu.make_async_remote_copy(
            src_ref=src, dst_ref=dst, send_sem=send, recv_sem=recv, device_id={AXIS: device}, device_id_type=pl.DeviceIdType.MESH
        )

    def place(kind):
        i = kind % 2
        if kind < B:
            return 2, 1 - i, i
        if kind < C:
            return sign[i], i, 2 + i
        if kind < OWN:
            return sign[i], 1 - i, i
        return 0, i, 3 - i

    spots = range(places.count)
    steps = [(k + i, p) for k in (A, B, C) for p in spots for i in range(2)] + [(OWN + h, p) for p in spots for h in (1, 0)]

    def load(kind, p):
        to, half, slot = place(kind)
        return pltpu.make_async_copy(places.rows(g, p, away(to, core), half), at(own, 4, p, slot), own_sem.at[p, slot])

    def give(kind, p):
        to, half, _ = place(kind)
        return remote(places.rows(g, p, away(to, 1 - core), half), at(par, 8, p, kind), par_send.at[p, kind], par_recv.at[p, kind], partner)

    def send(kind, p):
        slot = place(kind)[2]
        return remote(at(own, 4, p, slot), at(got, 6, p, kind), snd.at[p, kind], rcv.at[p, kind], beside[kind % 2])

    def start_load(t):
        kind, p = steps[t]
        if kind >= C:
            send(kind - C if kind < OWN else B + 1 - (kind - OWN), p).wait_send()
        load(kind, p).start()

    def add_up(kind, p):
        out = at(own, 4, p, place(kind)[2])
        terms = [out, at(par, 8, p, kind)]
        if C <= kind < OWN:
            terms.append(at(got, 6, p, kind - C))
        if kind >= OWN:
            i = 1 - (kind - OWN)
            terms += [at(got, 6, p, C + i), at(got, 6, p, B + 1 - i)]
        squares = acc[places.kinds.index(places.piece[p // places.layers])]

        def body(r, carry):
            rows = pl.ds(pl.multiple_of(r * GROUP, GROUP), GROUP)
            total = terms[0][rows, :].astype(jnp.float32)
            for one in terms[1:]:
                total = total + one[rows, :].astype(jnp.float32)
            total = total.astype(jnp.bfloat16)
            out[rows, :] = total
            if kind >= OWN:
                total = total.astype(jnp.float32)
                squares[...] += total * total
            return carry

        lax.fori_loop(0, places.half[p // places.layers] // GROUP, body, 0)

    def moments(p, h):
        return [
            pltpu.make_async_copy(places.own(m, p, h), at(mm, 2, p, h), mvw_sem.at[p, h, 0]),
            pltpu.make_async_copy(places.own(v, p, h), at(vv, 2, p, h), mvw_sem.at[p, h, 1]),
            pltpu.make_async_copy(places.rows(w, p, me, h), at(ww, 2, p, h), mvw_sem.at[p, h, 2]),
        ]

    for t in range(AHEAD):
        start_load(t)
    barrier = pltpu.get_barrier_semaphore()
    for device in (partner, *beside):
        pl.semaphore_signal(barrier, inc=1, device_id={AXIS: device}, device_id_type=pl.DeviceIdType.MESH)
    pl.semaphore_wait(barrier, 3)
    for t in range(FIRST):
        give(*steps[t]).start()
    for one in acc:
        one[...] = jnp.zeros_like(one)

    given = lambda t: min(FIRST + 2 * t, t + AHEAD, len(steps))
    for t, (kind, p) in enumerate(steps):
        load(kind, p).wait()
        give(kind, p).wait_recv()
        for ahead in range(given(t), given(t + 1)):
            give(*steps[ahead]).start()
        if C <= kind < OWN:
            send(kind - C, p).wait_recv()
        if kind >= OWN:
            i = 1 - (kind - OWN)
            send(B + 1 - i, p).wait_recv()
            send(C + i, p).wait_recv()
        add_up(kind, p)
        if kind < OWN:
            send(kind, p).start()
        if t + AHEAD < len(steps):
            start_load(t + AHEAD)
        if t == 2 * places.count:
            for q in spots:
                for h in range(2):
                    for copy in moments(q, h):
                        copy.start()

    sq[me] = jnp.full(sq.shape[1:], sum(jnp.sum(one[...]) for one in acc), jnp.float32)

    def tell(o, device):
        return remote(sq.at[device], sq.at[device], sq_send.at[o], sq_recv.at[o], lax.rem(me + o, n))

    for o in range(1, n):
        tell(o, me).start()
    for p in spots:
        for i in range(2):
            send(C + i, p).wait_send()
        for kind in range(8):
            give(kind, p).wait_send()
    for o in range(1, n):
        tell(o, lax.rem(me + (n - o), n)).wait_recv()
    for o in range(1, n):
        tell(o, me).wait_send()
    total = sq[0]
    for d in range(1, n):
        total = total + sq[d]
    factor_ref[...] = jnp.minimum(1.0, 0.5 * lax.rsqrt(total / count + 1e-30))

    def ahead(i, p, h):
        k = 2 * i + h
        return remote(at(ww, 2, p, h), places.rows(whole, p, me, h), snd.at[p, k], rcv.at[p, k], beside[i])

    def ahead_came(i, p, h):
        k = 2 * i + h
        here = places.rows(whole, p, away(-sign[i], core), h)
        return remote(here, here, snd.at[p, k], rcv.at[p, k], beside[i])

    def onward(i, p):
        here = places.rows(whole, p, away(-sign[i], core), 1 - i)
        there = last.at[i] if p == places.end else here
        return remote(here, there, snd.at[p, 4 + i], rcv.at[p, 4 + i], beside[i])

    def onward_came(i, p):
        here = last.at[i] if p == places.end else places.rows(whole, p, away(2, core), 1 - i)
        return remote(here, here, snd.at[p, 4 + i], rcv.at[p, 4 + i], beside[i])

    def extra(i):
        here = places.rows(whole, places.end, away(-sign[i], 1 - core), 1 - i)
        return remote(here, last.at[2 + i], snd.at[places.end, 3 * i], rcv.at[places.end, 3 * i], beside[i])

    def across(k, p):
        if k < 4:
            here = places.rows(whole, p, away(-sign[k // 2], core), k % 2)
        elif k < 6:
            here = places.rows(whole, p, away(2, core), 1 - (k - 4))
        else:
            here = places.rows(whole, p, me, k - 6)
        src = here if k < 6 else at(ww, 2, p, k - 6)
        return remote(src, here, par_send.at[p, k], par_recv.at[p, k], partner)

    def across_came(k, p):
        if k < 4:
            here = places.rows(whole, p, away(-sign[k // 2], 1 - core), k % 2)
        elif k < 6:
            here = places.rows(whole, p, away(2, 1 - core), 1 - (k - 4))
        else:
            here = places.rows(whole, p, partner, k - 6)
        return remote(here, here, par_send.at[p, k], par_recv.at[p, k], partner)

    def keep(p, h):
        return [pltpu.make_async_copy(at(ww, 2, p, h), places.rows(whole, p, me, h), own_sem.at[p, h])]

    def hand(p, h):
        kind, j = places.spot(p)
        return pltpu.make_async_copy(at(ww, 2, p, h), tails[2 * kind + h].at[j], mvw_sem.at[p, h, 0])

    def update(p, h):
        for copy in moments(p, h):
            copy.wait()
        gs, ms, vs, ws = at(own, 4, p, 3 - h), at(mm, 2, p, h), at(vv, 2, p, h), at(ww, 2, p, h)

        def body(r, carry):
            rows = pl.ds(pl.multiple_of(r * GROUP, GROUP), GROUP)
            grad = gs[rows, :].astype(jnp.float32) * factor_ref[0:1, 0:1]
            ws[rows, :], ms[rows, :], vs[rows, :] = adamw(ws[rows, :].astype(jnp.float32), ms[rows, :], vs[rows, :], grad)
            return carry

        lax.fori_loop(0, places.half[p // places.layers] // GROUP, body, 0)

    for p in spots:
        for h in (1, 0):
            update(p, h)
            ahead(1 - h, p, h).start()
            across(6 + h, p).start()
            for copy in keep(p, h):
                copy.start()
            if p in tail:
                hand(p, h).start()
    later = [p for p in spots if p not in tail]
    for p in later:
        for h in (0, 1):
            ahead(h, p, h).start()
    end, second = places.end, core == CORES - 1
    for p in spots[:-1]:
        for i in range(2):
            ahead_came(i, p, 1 - i).wait_recv()
            onward(i, p).start()
            across(2 * i + 1 - i, p).start()
    for i in range(2):
        ahead_came(i, end, 1 - i).wait_recv()
        across(2 * i + 1 - i, end).start()

    @pl.when(second)
    def _():
        for i in range(2):
            onward(i, end).start()
        for i in range(2):
            across_came(2 * i + 1 - i, end).wait_recv()
            extra(i).start()

    for p in later:
        for i in range(2):
            ahead_came(i, p, i).wait_recv()
            across(2 * i + i, p).start()
    for p in spots[:-1]:
        for i in range(2):
            onward_came(i, p).wait_recv()
            across(4 + i, p).start()

    @pl.when(second)
    def _():
        for i in range(2):
            for copy in (onward(i, end), extra(i)):
                copy.wait()

    @pl.when(jnp.logical_not(second))
    def _():
        for i in range(2):
            across_came(2 * i + 1 - i, end).wait_recv()

    for p in spots:
        for h in range(2):
            ahead(1 - h, p, h).wait_send()
            if p in later:
                ahead(h, p, h).wait_send()
            if p != end:
                onward(h, p).wait_send()
            for copy in keep(p, h):
                copy.wait()
            if p in tail:
                hand(p, h).wait()
        for k in range(8):
            if k in (0, 3) and p in tail or k in (4, 5) and p == places.end:
                continue
            across(k, p).wait_send()
            if k not in (1, 2) or p != end:
                across_came(k, p).wait_recv()


def gather_new(terms, weights, m, v, n, tail):
    shapes = [w.shape for w in weights]
    places = Places(n, shapes)
    count = float(sum(w.size for w in weights))
    anywhere, vmem = pl.BlockSpec(memory_space=pl.ANY), pl.BlockSpec(memory_space=pltpu.VMEM)
    out = [pltpu.HBM(s, jnp.bfloat16) for s in shapes]
    out += places.scratch(2, jnp.float32) * 2
    out += [jax.ShapeDtypeStruct((8, 128), jnp.float32)]
    out += [jax.ShapeDtypeStruct((len(m), *k), jnp.bfloat16) for m, k in zip(places.members, places.kinds) for _ in range(2)]
    out += [jax.ShapeDtypeStruct((4, *places.piece[-1]), jnp.bfloat16)]
    dma = pltpu.SemaphoreType.DMA
    half, nk = jnp.bfloat16, len(places.kinds)
    scratch = [
        *places.scratch(4, half), *places.scratch(8, half), *places.scratch(6, half),
        *places.scratch(2, half),
        *(pltpu.VMEM((GROUP, k[1]), jnp.float32) for k in places.kinds),
        pltpu.VMEM((n, 8, 128), jnp.float32),
        dma((places.count, 4)), dma((places.count, 8)), dma((places.count, 8)), dma((places.count, 6)), dma((places.count, 6)),
        dma((places.count, 2, 3)), dma((n,)), dma((n,)),
    ]
    got = pl.pallas_call(
        functools.partial(exchange, places, tail, count),
        out_shape=out,
        in_specs=[anywhere] * 12,
        out_specs=[anywhere] * 3 + [vmem] * (2 * nk + 1) + [anywhere] * (2 * nk + 1),
        scratch_shapes=scratch,
        compiler_params=pltpu.CompilerParams(collective_id=0, has_side_effects=True, vmem_limit_bytes=46 * 1000 * 1000),
        name="exchange",
    )(*terms, *weights, *m, *v)
    got_m, got_v, rest = got[3 : 3 + nk], got[3 + nk : 3 + 2 * nk], got[4 + 2 * nk :]
    return got[:3], got_m, got_v, rest[:-1], rest[-1]


def params(**more):
    return pltpu.CompilerParams(has_side_effects=False, **more)


def finish(places, tail, *refs):
    nk = len(places.kinds)
    parts, i = [], 0
    for size in (3, nk, nk, 3, 3, 3, nk, 1, 1, 1):
        parts.append(refs[i : i + size])
        i += size
    whole, mm, vv, out, new_m, new_v, slots, (in_sem,), (out_sem,), (put_sem,) = parts
    n = places.n
    chips = n // CORES
    chip = lax.div(lax.axis_index(AXIS), CORES)
    pieces = [(p, h) for p in range(places.count) for h in range(2)]

    def puts(p, h):
        refs = ((mm, new_m), (vv, new_v))
        return [pltpu.make_async_copy(places.at(a, 2, p, h), places.own(b, p, h), put_sem.at[p, h, j]) for j, (a, b) in enumerate(refs)]

    items = []
    for p, h in pieces:
        for k in range(chips):
            if p in tail and k == (1 if h else chips - 1) or p == places.end and k == 2:
                continue
            items += [(p, h, k, c) for c in range(CORES)]
    turn, of_kind = [], [[] for _ in range(nk)]
    for t, (p, *_) in enumerate(items):
        kind, _ = places.spot(p)
        turn.append((kind, len(of_kind[kind])))
        of_kind[kind].append(t)

    def ends(t):
        p, h, k, c = items[t]
        block = lax.rem(chip + k, chips) * CORES + c
        kind, u = turn[t]
        return places.rows(whole, p, block, h), slots[kind].at[u % SLOTS], places.rows(out, p, block, h), (kind, u % SLOTS)

    def read(t):
        src, slot, _, sem = ends(t)
        return pltpu.make_async_copy(src, slot, in_sem.at[sem])

    def write(t):
        _, slot, dst, sem = ends(t)
        return pltpu.make_async_copy(slot, dst, out_sem.at[sem])

    def start_read(t):
        kind, u = turn[t]
        if u >= SLOTS:
            write(of_kind[kind][u - SLOTS]).wait()
        read(t).start()

    for t in range(min(DEPTH, len(items))):
        start_read(t)
    done = 0
    for t in range(len(items)):
        read(t).wait()
        write(t).start()
        if t + DEPTH < len(items):
            start_read(t + DEPTH)
        while done * len(items) < (t + 1) * len(pieces) and done < len(pieces):
            for copy in puts(*pieces[done]):
                copy.start()
            done += 1
    for kind in range(nk):
        for t in of_kind[kind][-SLOTS:]:
            write(t).wait()
    for p, h in pieces:
        for copy in puts(p, h):
            copy.wait()


def finish_all(places, tail, whole, mm, vv, m, v):
    anywhere, vmem = pl.BlockSpec(memory_space=pl.ANY), pl.BlockSpec(memory_space=pltpu.VMEM)
    dma = pltpu.SemaphoreType.DMA
    nk = len(places.kinds)
    size = sum(w.size for w in whole)
    mine = sum(one.size for one in m)
    whole = [pltpu.with_memory_space_constraint(w, pltpu.HBM) for w in whole]
    mm, vv = ([pltpu.with_memory_space_constraint(one, pltpu.VMEM) for one in x] for x in (mm, vv))
    return pl.pallas_call(
        functools.partial(finish, places, tail),
        out_shape=[jax.ShapeDtypeStruct(a.shape, a.dtype) for a in (*whole, *m, *v)],
        in_specs=[anywhere] * 3 + [vmem] * (2 * nk),
        out_specs=[anywhere] * 9,
        scratch_shapes=[
            *(pltpu.VMEM((SLOTS, *k), jnp.bfloat16) for k in places.kinds),
            dma((nk, SLOTS)), dma((nk, SLOTS)), dma((places.count, 2, 2)),
        ],
        compiler_params=params(vmem_limit_bytes=24 * 1024 * 1024),
        cost_estimate=pl.CostEstimate(flops=size * 100, bytes_accessed=size * 4 + mine * 8, transcendentals=0),
        name="finish",
    )(*whole, *mm, *vv)


def place_late(places, spots, *refs):
    k = len(spots)
    arrays, out, sem = refs[:k], refs[k + 3 : k + 6], refs[k + 6]
    chips = places.n // CORES
    me = lax.axis_index(AXIS)
    core, chip = lax.rem(me, CORES), lax.div(me, CORES)
    jobs = {}
    for array, (only, pieces) in zip(arrays, spots):
        for j, (p, h, away, which) in enumerate(pieces):
            block = lax.rem(chip + (away + chips), chips) * CORES + (lax.rem(core + which[1], CORES) if which[0] else which[1])
            mine = jobs.setdefault(only, [])
            mine.append(pltpu.make_async_copy(array.at[j], places.rows(out, p, block, h), sem.at[sum(len(x) for x in jobs.values())]))

    for only, copies in jobs.items():

        def run():
            for copy in copies:
                copy.start()
            for copy in copies:
                copy.wait()

        run() if only is None else pl.when(core == only)(run)


def place_all(places, spots, arrays, out):
    anywhere, vmem = pl.BlockSpec(memory_space=pl.ANY), pl.BlockSpec(memory_space=pltpu.VMEM)
    k = len(spots)
    return pl.pallas_call(
        functools.partial(place_late, places, spots),
        out_shape=[jax.ShapeDtypeStruct(w.shape, w.dtype) for w in out],
        in_specs=[vmem] * k + [anywhere] * 3,
        out_specs=[anywhere] * 3,
        input_output_aliases={k + j: j for j in range(3)},
        scratch_shapes=[pltpu.SemaphoreType.DMA((sum(len(one) for _, one in spots),))],
        compiler_params=params(vmem_limit_bytes=16 * 1024 * 1024),
        cost_estimate=pl.CostEstimate(flops=10**7, bytes_accessed=sum(x.size for x in arrays) * 4, transcendentals=0),
        name="place_late",
    )(*arrays, *out)


def solution(mesh):
    n = mesh.shape[AXIS]
    chips = n // CORES

    def step(*arrays):
        terms, weights, m, v = (arrays[i : i + 3] for i in (0, 3, 6, 9))
        places = Places(n, [w.shape for w in weights])
        tail = list(range(places.count))
        whole, mm, vv, late, last = gather_new([t[0] for t in terms], weights, m, v, n, tail)
        kinds = range(len(places.kinds))
        shift = [[(j, (j // CORES + s) % chips * CORES + j % CORES) for j in range(n)] for s in (1, -1)]
        swap = [(j, j // CORES * CORES + (CORES - 1 - j % CORES)) for j in range(n)]
        came = []
        for k in kinds:
            came.append([lax.ppermute(late[2 * k + h], AXIS, shift[h]) for h in range(2)])
        last_swapped = lax.ppermute(last, AXIS, swap)
        *out, m0, m1, m2, v0, v1, v2 = finish_all(places, tail, whole, mm, vv, m, v)
        own, other = (True, 0), (True, 1)
        spots = lambda k, which: [(None, [(p, h, -1 if h == 0 else 1, which) for p in places.members[k]]) for h in range(2)]
        ends = [(places.end, 1 - i, 2, (False, c)) for c in (1, 0) for i in range(2)]
        for k in kinds:
            here, out = lax.optimization_barrier((came[k], out))
            swapped = [lax.ppermute(piece, AXIS, swap) for piece in here]
            if k == 0:
                out = place_all(places, [*spots(k, own), (1, ends), (0, ends)], [*here, last, last_swapped], out)
            else:
                out = place_all(places, spots(k, own), here, out)
            out = place_all(places, spots(k, other), swapped, out)
        return (*out, m0, m1, m2, v0, v1, v2)

    all_of, cut = P(None, None, None), P(None, AXIS, None)
    return jax.shard_map(
        step,
        mesh=mesh,
        in_specs=(P(("rep", AXIS), None, None, None),) * 3 + (all_of,) * 3 + (cut,) * 6,
        out_specs=(P("rep", None, None),) * 3 + (P("rep", AXIS, None),) * 6,
        check_vma=False,
    )
```

```python
import functools

import jax
import jax.numpy as jnp
from jax import lax
from jax.experimental import pallas as pl
from jax.experimental.pallas import tpu as pltpu
from jax.sharding import PartitionSpec as P


AXIS = "dp"
CORES = 2
AHEAD = 6
GROUP = 16
RING = 8
SLOTS, DEPTH = 16, 8
A, B, C, OWN = 0, 2, 4, 6


def adamw(w, m, v, g):
    m = 0.9 * m + 0.1 * g
    v = 0.95 * v + 0.05 * g * g
    step = m * lax.rsqrt(v + 1e-8) + 0.1 * w
    return (w - 0.02 * step).astype(jnp.bfloat16), m, v


class Places:
    def __init__(self, n, shapes):
        self.n = n
        self.layers = shapes[0][0]
        self.half = [rows // n // 2 for _, rows, _ in shapes]
        self.piece = [(h, cols) for h, (_, _, cols) in zip(self.half, shapes)]
        self.count = len(shapes) * self.layers
        self.kinds = sorted(set(self.piece), key=self.piece.index)
        self.members = [[p for p in range(self.count) if self.piece[p // self.layers] == k] for k in self.kinds]

        self.end = self.count - 1
        self.groups = [*self.members[:-1], self.members[-1][:-1], [self.end]]

    def scratch(self, slots, dtype):
        return [pltpu.VMEM((len(m) * slots, *k), dtype) for m, k in zip(self.members, self.kinds)]

    def spot(self, p):
        kind = self.kinds.index(self.piece[p // self.layers])
        return kind, self.members[kind].index(p)

    def at(self, buffers, slots, p, slot):
        kind, j = self.spot(p)
        return buffers[kind].at[j * slots + slot]

    def rows(self, refs, p, block, half):
        w = p // self.layers
        start = pl.multiple_of((block * 2 + half) * self.half[w], GROUP)
        return refs[w].at[p % self.layers, pl.ds(start, self.half[w]), :]

    def own(self, refs, p, half):
        w = p // self.layers
        return refs[w].at[p % self.layers, pl.ds(half * self.half[w], self.half[w]), :]


def exchange(places, count, *refs):
    nk = len(places.kinds)
    names = (3, 3, 3, 3, 3, nk, nk, 1, 2 * len(places.groups) + 1, nk, nk, nk, nk, *(1,) * 10)
    parts, i = [], 0
    for size in names:
        parts.append(refs[i : i + size])
        i += size
    g, w, m, v, whole, mm, vv, (factor_ref,), (*tails, last) = parts[:9]
    own, par, got, ww = parts[9:13]
    (sq,), (own_sem,), (first_sem,), (par_recv,), (came_sem,), (pass_sem,), (all_sem,), (extra_send,), (extra_recv,), (end_recv,) = parts[13:]

    n, at, end = places.n, places.at, places.end
    chips = n // CORES
    me = lax.axis_index(AXIS)
    core, chip = lax.rem(me, CORES), lax.div(me, CORES)
    away = lambda k, core: lax.rem(chip + (k + chips), chips) * CORES + core
    partner = away(0, 1 - core)
    sign = (1, -1)
    beside = [away(s, core) for s in sign]
    second = core == CORES - 1
    kind_of = lambda p: places.spot(p)[0]
    each = range(nk)

    def remote(src, dst, send, recv, device):
        return pltpu.make_async_remote_copy(
            src_ref=src, dst_ref=dst, send_sem=send, recv_sem=recv, device_id={AXIS: device}, device_id_type=pl.DeviceIdType.MESH
        )

    SUM_GIVEN, SUM_A, SUM_B, SUM_C, B_CAME, M, V, W, SENT, ACROSS, ACROSS_CAME, KEPT, HANDED, TOLD, HEARD = range(15)
    shared = lambda what, p: all_sem.at[what, kind_of(p)]

    def all_of(what, kind, ref, size):
        sem, ref = all_sem.at[what, kind], ref if size is None else ref.at[pl.ds(0, size)]
        remote(ref, ref, sem, sem, partner).wait_recv()

    def place(kind):
        i = kind % 2
        if kind < B:
            return 2, 1 - i, i
        if kind < C:
            return sign[i], i, 2 + i
        if kind < OWN:
            return sign[i], 1 - i, i
        return 0, i, 3 - i

    spots = range(places.count)
    steps = [(k + i, p) for k in (A, B, C) for p in spots for i in range(2)] + [(OWN + h, p) for p in spots for h in (1, 0)]
    groups = lambda p: places.half[p // places.layers] // GROUP
    part = lambda ref, r: ref if r is None else ref.at[pl.ds(r * GROUP, GROUP), :]

    def load(t):
        kind, p = steps[t]
        to, half, slot = place(kind)
        return pltpu.make_async_copy(places.rows(g, p, away(to, core), half), at(own, 4, p, slot), own_sem.at[t % RING])

    def give(t, r=None):
        kind, p = steps[t]
        to, half, _ = place(kind)
        recv = par_recv.at[t % (2 * RING)] if r is None else first_sem.at[t, r]
        src, dst = part(places.rows(g, p, away(to, 1 - core), half), r), part(at(par, 8, p, kind), r)
        return remote(src, dst, shared(SUM_GIVEN, p), recv, partner)

    def send(kind, p, r=None):
        what, i = (SUM_A, SUM_B, SUM_C)[kind // 2], kind % 2
        recv = (came_sem.at[p, i], shared(B_CAME, p), pass_sem.at[p, i])[kind // 2]
        return remote(part(at(own, 4, p, place(kind)[2]), r), part(at(got, 6, p, kind), r), shared(what, p), recv, beside[i])

    def start_load(t):
        if steps[t] in ((C, 0), (OWN + 1, 0)):
            for k in each:
                all_of(SUM_A if steps[t][0] < OWN else SUM_B, k, own[k], 2 * len(places.members[k]))
        load(t).start()

    def add_up(kind, p, first, last):
        out = at(own, 4, p, place(kind)[2])
        terms = [out, at(par, 8, p, kind)]
        if C <= kind < OWN:
            terms.append(at(got, 6, p, kind - C))
        if kind >= OWN:
            i = 1 - (kind - OWN)
            terms += [at(got, 6, p, C + i), at(got, 6, p, B + 1 - i)]

        def body(r, carry):
            rows = pl.ds(pl.multiple_of(r * GROUP, GROUP), GROUP)
            total = terms[0][rows, :].astype(jnp.float32)
            for one in terms[1:]:
                total = total + one[rows, :].astype(jnp.float32)
            total = total.astype(jnp.bfloat16)
            out[rows, :] = total
            if kind >= OWN:
                total = total.astype(jnp.float32)
                total = total * total
                tiles = [total[a : a + 8, b : b + 128] for a in range(0, GROUP, 8) for b in range(0, total.shape[1], 128)]
                sums = [sum(tiles[j::4]) for j in range(4)]
                carry = carry + ((sums[0] + sums[1]) + (sums[2] + sums[3]))
            return carry

        if kind < OWN:
            lax.fori_loop(first, last, body, 0)
        else:
            sq[me] = lax.fori_loop(first, last, body, sq[me])

    for t in range(AHEAD):
        start_load(t)
    barrier = pltpu.get_barrier_semaphore()
    for device in (partner, *beside):
        pl.semaphore_signal(barrier, inc=1, device_id={AXIS: device}, device_id_type=pl.DeviceIdType.MESH)
    pl.semaphore_wait(barrier, 3)
    for r in range(groups(0)):
        for t in range(2):
            give(t, r).start()
    for t in range(2, AHEAD):
        give(t).start()
    sq[me] = jnp.zeros(sq.shape[1:], jnp.float32)

    for r in range(groups(0)):
        for t in range(2):
            if r == 0:
                load(t).wait()
            give(t, r).wait_recv()
            add_up(*steps[t], r, r + 1)
            send(*steps[t], r).start()
    for t, (kind, p) in enumerate(steps):
        if t + AHEAD < len(steps):
            give(t + AHEAD).start()
        if t >= 2:
            load(t).wait()
            give(t).wait_recv()
            if C <= kind < OWN:
                send(kind - C, p).wait_recv()
            if (kind, p) == (OWN + 1, 0):
                for k in each:
                    all_of(B_CAME, k, got[k], 2 * len(places.members[k]))
            if kind >= OWN:
                send(C + 1 - (kind - OWN), p).wait_recv()
            add_up(kind, p, 0, groups(p))
            if kind < OWN:
                send(kind, p).start()
        if t + AHEAD < len(steps):
            start_load(t + AHEAD)
        if t == 2 * places.count:
            for q in spots:
                for h in range(2):
                    pltpu.make_async_copy(places.own(m, q, h), at(mm, 2, q, h), shared(M, q)).start()
                    pltpu.make_async_copy(places.own(v, q, h), at(vv, 2, q, h), shared(V, q)).start()
                    pltpu.make_async_copy(places.rows(w, q, me, h), at(ww, 2, q, h), shared(W, q)).start()

    for o in range(1, n):
        remote(sq.at[me], sq.at[me], all_sem.at[TOLD, 0], all_sem.at[HEARD, 0], lax.rem(me + o, n)).start()
    for k in each:
        all_of(SUM_C, k, own[k], 2 * len(places.members[k]))
        all_of(SUM_GIVEN, k, par[k], None)
        for what, buffers in ((M, mm), (V, vv), (W, ww)):
            all_of(what, k, buffers[k], None)
    all_of(HEARD, 0, sq, n - 1)
    total = sq[0]
    for d in range(1, n):
        total = total + sq[d]
    total = jnp.full(factor_ref.shape, jnp.sum(total), jnp.float32)
    factor_ref[...] = jnp.minimum(1.0, 0.5 * lax.rsqrt(total / count + 1e-30))

    def ahead(i, p, h, r=None):
        there = part(places.rows(whole, p, me, h), r)
        return remote(part(at(ww, 2, p, h), r), there, shared(SENT, p), came_sem.at[p, i], beside[i])

    def ahead_came(i, p):
        here = places.rows(whole, p, away(-sign[i], core), 1 - i)
        return remote(here, here, shared(SENT, p), came_sem.at[p, i], beside[i])

    def onward(i, p):
        here = places.rows(whole, p, away(-sign[i], core), 1 - i)
        if p == end:
            return remote(here, last.at[i], extra_send.at[i], pass_sem.at[p, i], beside[i])
        return remote(here, here, shared(SENT, p), pass_sem.at[p, i], beside[i])

    def onward_came(i, p):
        here = places.rows(whole, p, away(2, core), 1 - i)
        return remote(here, here, shared(SENT, p), pass_sem.at[p, i], beside[i])

    def extra(i):
        here = places.rows(whole, end, away(-sign[i], 1 - core), 1 - i)
        return remote(here, last.at[2 + i], extra_send.at[2 + i], extra_recv.at[i], beside[i])

    def across(k, p):
        if k < 2:
            here = places.rows(whole, p, away(-sign[k], core), 1 - k)
        elif k < 4:
            here = places.rows(whole, p, away(2, core), 1 - (k - 2))
        else:
            here = places.rows(whole, p, me, k - 4)
        src = here if k < 4 else at(ww, 2, p, k - 4)
        recv = end_recv.at[k] if p == end and k < 2 else shared(ACROSS_CAME, p)
        return remote(src, here, shared(ACROSS, p), recv, partner)

    def side_came_across(i):
        here = places.rows(whole, end, away(-sign[i], 1 - core), 1 - i)
        return remote(here, here, end_recv.at[i], end_recv.at[i], partner)

    def update(p, h, first, last):
        gs, ms, vs, ws = at(own, 4, p, 3 - h), at(mm, 2, p, h), at(vv, 2, p, h), at(ww, 2, p, h)

        def body(r, carry):
            rows = pl.ds(pl.multiple_of(r * GROUP, GROUP), GROUP)
            grad = gs[rows, :].astype(jnp.float32) * factor_ref[0:1, 0:1]
            ws[rows, :], ms[rows, :], vs[rows, :] = adamw(ws[rows, :].astype(jnp.float32), ms[rows, :], vs[rows, :], grad)
            return carry

        lax.fori_loop(first, last, body, 0)

    for r in range(groups(0)):
        for h in (1, 0):
            update(0, h, r, r + 1)
            ahead(1 - h, 0, h, r).start()
    for p in spots:
        for h in (1, 0):
            if p:
                update(p, h, 0, groups(p))
                ahead(1 - h, p, h).start()
            across(4 + h, p).start()
            pltpu.make_async_copy(at(ww, 2, p, h), places.rows(whole, p, me, h), shared(KEPT, p)).start()
            k, j = next((k, one.index(p)) for k, one in enumerate(places.groups) if p in one)
            pltpu.make_async_copy(at(ww, 2, p, h), tails[2 * k + h].at[j], shared(HANDED, p)).start()
    for p in spots:
        for i in range(2):
            ahead_came(i, p).wait_recv()
            if p != end:
                onward(i, p).start()
            across(i, p).start()

    @pl.when(second)
    def _():
        for i in range(2):
            onward(i, end).start()
        for i in range(2):
            side_came_across(i).wait_recv()
            extra(i).start()

    for p in spots[:-1]:
        for i in range(2):
            onward_came(i, p).wait_recv()
            across(2 + i, p).start()
    for k in each:
        members = len(places.members[k])
        ends = 1 if k == kind_of(end) else 0
        all_of(SENT, k, own[k], 4 * members - 2 * ends)
        all_of(ACROSS, k, par[k], 6 * members - 2 * ends)
        all_of(ACROSS_CAME, k, par[k], 6 * members - 4 * ends)
        all_of(KEPT, k, ww[k], None)
        all_of(HANDED, k, ww[k], None)
    all_of(TOLD, 0, sq, n - 1)

    @pl.when(second)
    def _():
        for i in range(2):
            for copy in (onward(i, end), extra(i)):
                copy.wait()

    @pl.when(jnp.logical_not(second))
    def _():
        for i in range(2):
            side_came_across(i).wait_recv()


def gather_new(terms, weights, m, v, n):
    shapes = [w.shape for w in weights]
    places = Places(n, shapes)
    count = float(sum(w.size for w in weights))
    anywhere, vmem = pl.BlockSpec(memory_space=pl.ANY), pl.BlockSpec(memory_space=pltpu.VMEM)
    out = [pltpu.HBM(s, jnp.bfloat16) for s in shapes]
    out += places.scratch(2, jnp.float32) * 2
    out += [jax.ShapeDtypeStruct((8, 128), jnp.float32)]
    out += [jax.ShapeDtypeStruct((len(one), *places.piece[one[0] // places.layers]), jnp.bfloat16) for one in places.groups for _ in range(2)]
    out += [jax.ShapeDtypeStruct((4, *places.piece[-1]), jnp.bfloat16)]
    dma = pltpu.SemaphoreType.DMA
    half, nk = jnp.bfloat16, len(places.kinds)
    scratch = [
        *places.scratch(4, half), *places.scratch(8, half), *places.scratch(6, half),
        *places.scratch(2, half),
        pltpu.VMEM((n, 8, 128), jnp.float32),
        dma((RING,)), dma((2, places.half[0] // GROUP)), dma((2 * RING,)), dma((places.count, 2)), dma((places.count, 2)),
        dma((15, nk)), dma((4,)), dma((2,)), dma((2,)),
    ]
    got = pl.pallas_call(
        functools.partial(exchange, places, count),
        out_shape=out,
        in_specs=[anywhere] * 12,
        out_specs=[anywhere] * 3 + [vmem] * (2 * nk + 1) + [anywhere] * (2 * len(places.groups) + 1),
        scratch_shapes=scratch,
        compiler_params=pltpu.CompilerParams(collective_id=0, has_side_effects=True, vmem_limit_bytes=46 * 1000 * 1000),
        name="exchange",
    )(*terms, *weights, *m, *v)
    got_m, got_v, rest = got[3 : 3 + nk], got[3 + nk : 3 + 2 * nk], got[4 + 2 * nk :]
    return got[:3], got_m, got_v, rest[:-1], rest[-1]


def params(**more):
    return pltpu.CompilerParams(has_side_effects=False, **more)


def finish(places, tail, *refs):
    nk = len(places.kinds)
    parts, i = [], 0
    for size in (3, nk, nk, 3, 3, 3, nk, 1, 1, 1):
        parts.append(refs[i : i + size])
        i += size
    whole, mm, vv, out, new_m, new_v, slots, (in_sem,), (out_sem,), (put_sem,) = parts
    n = places.n
    chips = n // CORES
    chip = lax.div(lax.axis_index(AXIS), CORES)
    pieces = [(p, h) for p in range(places.count) for h in range(2)]

    def puts(p, h):
        refs = ((mm, new_m), (vv, new_v))
        return [pltpu.make_async_copy(places.at(a, 2, p, h), places.own(b, p, h), put_sem.at[j, places.spot(p)[0]]) for j, (a, b) in enumerate(refs)]

    items = []
    for p, h in pieces:
        for k in range(chips):
            if p in tail and k == (1 if h else chips - 1) or p == places.end and k == 2:
                continue
            items += [(p, h, k, c) for c in range(CORES)]
    turn, of_kind = [], [[] for _ in range(nk)]
    for t, (p, *_) in enumerate(items):
        kind, _ = places.spot(p)
        turn.append((kind, len(of_kind[kind])))
        of_kind[kind].append(t)

    def ends(t):
        p, h, k, c = items[t]
        block = lax.rem(chip + k, chips) * CORES + c
        kind, u = turn[t]
        return places.rows(whole, p, block, h), slots[kind].at[u % SLOTS], places.rows(out, p, block, h), (kind, u % SLOTS)

    def read(t):
        src, slot, _, sem = ends(t)
        return pltpu.make_async_copy(src, slot, in_sem.at[sem])

    def write(t):
        _, slot, dst, sem = ends(t)
        return pltpu.make_async_copy(slot, dst, out_sem.at[sem])

    def start_read(t):
        kind, u = turn[t]
        if u >= SLOTS:
            write(of_kind[kind][u - SLOTS]).wait()
        read(t).start()

    for t in range(min(DEPTH, len(items))):
        start_read(t)
    done = 0
    for t in range(len(items)):
        read(t).wait()
        write(t).start()
        if t + DEPTH < len(items):
            start_read(t + DEPTH)
        while done * len(items) < (t + 1) * len(pieces) and done < len(pieces):
            for copy in puts(*pieces[done]):
                copy.start()
            done += 1
    for kind in range(nk):
        for t in of_kind[kind][-SLOTS:]:
            write(t).wait()
    for kind in range(nk):
        for j, one in enumerate((mm, vv)):
            pltpu.make_async_copy(one[kind], one[kind], put_sem.at[j, kind]).wait()


def finish_all(places, tail, whole, mm, vv, m, v):
    anywhere, vmem = pl.BlockSpec(memory_space=pl.ANY), pl.BlockSpec(memory_space=pltpu.VMEM)
    dma = pltpu.SemaphoreType.DMA
    nk = len(places.kinds)
    size = sum(w.size for w in whole)
    mine = sum(one.size for one in m)
    whole = [pltpu.with_memory_space_constraint(w, pltpu.HBM) for w in whole]
    mm, vv = ([pltpu.with_memory_space_constraint(one, pltpu.VMEM) for one in x] for x in (mm, vv))
    return pl.pallas_call(
        functools.partial(finish, places, tail),
        out_shape=[jax.ShapeDtypeStruct(a.shape, a.dtype) for a in (*whole, *m, *v)],
        in_specs=[anywhere] * 3 + [vmem] * (2 * nk),
        out_specs=[anywhere] * 9,
        scratch_shapes=[
            *(pltpu.VMEM((SLOTS, *k), jnp.bfloat16) for k in places.kinds),
            dma((nk, SLOTS)), dma((nk, SLOTS)), dma((2, nk)),
        ],
        compiler_params=params(vmem_limit_bytes=24 * 1024 * 1024),
        cost_estimate=pl.CostEstimate(flops=size * 100, bytes_accessed=size * 4 + mine * 8, transcendentals=0),
        name="finish",
    )(*whole, *mm, *vv)


def place_late(places, spots, *refs):
    k = len(spots)
    arrays, out, sem = refs[:k], refs[k + 3 : k + 6], refs[k + 6]
    chips = places.n // CORES
    me = lax.axis_index(AXIS)
    core, chip = lax.rem(me, CORES), lax.div(me, CORES)
    jobs = {}
    for array, (only, pieces) in zip(arrays, spots):
        for j, (p, h, away, which) in enumerate(pieces):
            block = lax.rem(chip + (away + chips), chips) * CORES + (lax.rem(core + which[1], CORES) if which[0] else which[1])
            mine = jobs.setdefault(only, [])
            mine.append(pltpu.make_async_copy(array.at[j], places.rows(out, p, block, h), sem.at[sum(len(x) for x in jobs.values())]))

    for only, copies in jobs.items():

        def run():
            for copy in copies:
                copy.start()
            for copy in copies:
                copy.wait()

        run() if only is None else pl.when(core == only)(run)


def place_all(places, spots, arrays, out):
    anywhere, vmem = pl.BlockSpec(memory_space=pl.ANY), pl.BlockSpec(memory_space=pltpu.VMEM)
    k = len(spots)
    return pl.pallas_call(
        functools.partial(place_late, places, spots),
        out_shape=[jax.ShapeDtypeStruct(w.shape, w.dtype) for w in out],
        in_specs=[vmem] * k + [anywhere] * 3,
        out_specs=[anywhere] * 3,
        input_output_aliases={k + j: j for j in range(3)},
        scratch_shapes=[pltpu.SemaphoreType.DMA((sum(len(one) for _, one in spots),))],
        compiler_params=params(vmem_limit_bytes=16 * 1024 * 1024),
        cost_estimate=pl.CostEstimate(flops=10**7, bytes_accessed=sum(x.size for x in arrays) * 4, transcendentals=0),
        name="place_late",
    )(*arrays, *out)


def solution(mesh):
    n = mesh.shape[AXIS]
    chips = n // CORES

    def step(*arrays):
        terms, weights, m, v = (arrays[i : i + 3] for i in (0, 3, 6, 9))
        places = Places(n, [w.shape for w in weights])
        tail = list(range(places.count))
        whole, mm, vv, late, last = gather_new([t[0] for t in terms], weights, m, v, n)
        groups = range(len(places.groups))
        shift = [[(j, (j // CORES + s) % chips * CORES + j % CORES) for j in range(n)] for s in (1, -1)]
        swap = [(j, j // CORES * CORES + (CORES - 1 - j % CORES)) for j in range(n)]
        came = []
        for k in groups:
            came.append([lax.ppermute(late[2 * k + h], AXIS, shift[h]) for h in range(2)])
        last_swapped = lax.ppermute(last, AXIS, swap)
        *out, m0, m1, m2, v0, v1, v2 = finish_all(places, tail, whole, mm, vv, m, v)
        own, other = (True, 0), (True, 1)
        spots = lambda k, which: [(None, [(p, h, -1 if h == 0 else 1, which) for p in places.groups[k]]) for h in range(2)]
        ends = [(places.end, 1 - i, 2, (False, c)) for c in (1, 0) for i in range(2)]
        for k in groups:
            here, out = lax.optimization_barrier((came[k], out))
            swapped = [lax.ppermute(piece, AXIS, swap) for piece in here]
            if k == 0:
                out = place_all(places, [*spots(k, own), (1, ends), (0, ends)], [*here, last, last_swapped], out)
            else:
                out = place_all(places, spots(k, own), here, out)
            out = place_all(places, spots(k, other), swapped, out)
        return (*out, m0, m1, m2, v0, v1, v2)

    all_of, cut = P(None, None, None), P(None, AXIS, None)
    return jax.shard_map(
        step,
        mesh=mesh,
        in_specs=(P(("rep", AXIS), None, None, None),) * 3 + (all_of,) * 3 + (cut,) * 6,
        out_specs=(P("rep", None, None),) * 3 + (P("rep", AXIS, None),) * 6,
        check_vma=False,
    )
```

```python
import functools

import jax
import jax.numpy as jnp
from jax import lax
from jax.experimental import pallas as pl
from jax.experimental.pallas import tpu as pltpu
from jax.sharding import PartitionSpec as P


AXIS = "dp"
CORES = 2
AHEAD = 6
GROUP = 16
RING = 8
SLOTS, DEPTH = 16, 8
A, B, C, OWN = 0, 2, 4, 6


def adamw(w, m, v, g):
    m = 0.9 * m + 0.1 * g
    v = 0.95 * v + 0.05 * g * g
    step = m * lax.rsqrt(v + 1e-8) + 0.1 * w
    return (w - 0.02 * step).astype(jnp.bfloat16), m, v


class Places:
    def __init__(self, n, shapes):
        self.n = n
        self.layers = shapes[0][0]
        self.half = [rows // n // 2 for _, rows, _ in shapes]
        self.piece = [(h, cols) for h, (_, _, cols) in zip(self.half, shapes)]
        self.count = len(shapes) * self.layers
        self.kinds = sorted(set(self.piece), key=self.piece.index)
        self.members = [[p for p in range(self.count) if self.piece[p // self.layers] == k] for k in self.kinds]

        self.end = self.count - 1
        whole = [[(p, 0, k[0]) for p in m] for m, k in zip(self.members, self.kinds)]
        rows = self.kinds[-1][0]
        cut = (rows // GROUP + 1) // 2 * GROUP
        self.groups = [*whole[:-1], whole[-1][:-1] + [(self.end, 0, cut)], [(self.end, cut, rows - cut)]]
        self.late = [((sum(r for _, _, r in one), self.piece[one[0][0] // self.layers][1]), one) for one in self.groups]

    def cuts(self):
        n = self.kinds[-1][0] // GROUP
        size = -(-n // 4)
        return [(a, min(size, n - a)) for a in range(0, n, size)]

    def scratch(self, slots, dtype):
        return [pltpu.VMEM((len(m) * slots, *k), dtype) for m, k in zip(self.members, self.kinds)]

    def spot(self, p):
        kind = self.kinds.index(self.piece[p // self.layers])
        return kind, self.members[kind].index(p)

    def at(self, buffers, slots, p, slot):
        kind, j = self.spot(p)
        return buffers[kind].at[j * slots + slot]

    def rows(self, refs, p, block, half, first=0, size=None):
        w = p // self.layers
        start = pl.multiple_of((block * 2 + half) * self.half[w] + first, GROUP)
        return refs[w].at[p % self.layers, pl.ds(start, self.half[w] if size is None else size), :]

    def own(self, refs, p, half):
        w = p // self.layers
        return refs[w].at[p % self.layers, pl.ds(half * self.half[w], self.half[w]), :]


def exchange(places, count, *refs):
    nk = len(places.kinds)
    names = (3, 3, 3, 3, 3, nk, nk, 1, 2 * len(places.groups) + 1, nk, nk, nk, nk, *(1,) * 11)
    parts, i = [], 0
    for size in names:
        parts.append(refs[i : i + size])
        i += size
    g, w, m, v, whole, mm, vv, (factor_ref,), (*tails, last) = parts[:9]
    own, par, got, ww = parts[9:13]
    (sq,), (own_sem,), (first_sem,), (par_recv,), (came_sem,), (pass_sem,), (all_sem,), (extra_send,), (extra_recv,), (end_recv,), (cut_sem,) = parts[13:]

    n, at, end = places.n, places.at, places.end
    prev = end - 1
    chips = n // CORES
    me = lax.axis_index(AXIS)
    core, chip = lax.rem(me, CORES), lax.div(me, CORES)
    away = lambda k, core: lax.rem(chip + (k + chips), chips) * CORES + core
    partner = away(0, 1 - core)
    sign = (1, -1)
    beside = [away(s, core) for s in sign]
    second = core == CORES - 1
    kind_of = lambda p: places.spot(p)[0]
    each = range(nk)

    def remote(src, dst, send, recv, device):
        return pltpu.make_async_remote_copy(
            src_ref=src, dst_ref=dst, send_sem=send, recv_sem=recv, device_id={AXIS: device}, device_id_type=pl.DeviceIdType.MESH
        )

    SUM_GIVEN, SUM_A, SUM_B, SUM_C, B_CAME, M, V, W, SENT, ACROSS, ACROSS_CAME, KEPT, HANDED, TOLD, HEARD = range(15)
    shared = lambda what, p: all_sem.at[what, kind_of(p)]

    def all_of(what, kind, ref, size):
        sem, ref = all_sem.at[what, kind], ref if size is None else ref.at[pl.ds(0, size)]
        remote(ref, ref, sem, sem, partner).wait_recv()

    def place(kind):
        i = kind % 2
        if kind < B:
            return 2, 1 - i, i
        if kind < C:
            return sign[i], i, 2 + i
        if kind < OWN:
            return sign[i], 1 - i, i
        return 0, i, 3 - i

    spots = range(places.count)
    steps = [(k + i, p) for k in (A, B, C) for p in spots for i in range(2)] + [(OWN + h, p) for p in spots for h in (1, 0)]
    groups = lambda p: places.half[p // places.layers] // GROUP
    cuts = places.cuts()
    part = lambda ref, r: ref if r is None else ref.at[pl.ds(r * GROUP, GROUP), :]

    def load(t):
        kind, p = steps[t]
        to, half, slot = place(kind)
        return pltpu.make_async_copy(places.rows(g, p, away(to, core), half), at(own, 4, p, slot), own_sem.at[t % RING])

    def give(t, r=None):
        kind, p = steps[t]
        to, half, _ = place(kind)
        recv = par_recv.at[t % (2 * RING)] if r is None else first_sem.at[t, r]
        src, dst = part(places.rows(g, p, away(to, 1 - core), half), r), part(at(par, 8, p, kind), r)
        return remote(src, dst, shared(SUM_GIVEN, p), recv, partner)

    def send(kind, p, r=None, rows=None):
        what, i = (SUM_A, SUM_B, SUM_C)[kind // 2], kind % 2
        recv = (came_sem.at[p, i], shared(B_CAME, p), pass_sem.at[p, i])[kind // 2]
        src, dst = part(at(own, 4, p, place(kind)[2]), r), part(at(got, 6, p, kind), r)
        if rows is not None:
            first, size = cuts[rows]
            src, dst = (ref.at[pl.ds(first * GROUP, size * GROUP), :] for ref in (src, dst))
            recv = cut_sem.at[i, rows]
        return remote(src, dst, shared(what, p), recv, beside[i])

    def start_load(t):
        if steps[t] in ((C, 0), (OWN + 1, 0)):
            for k in each:
                all_of(SUM_A if steps[t][0] < OWN else SUM_B, k, own[k], 2 * len(places.members[k]))
        load(t).start()

    def add_up(kind, p, first, last):
        out = at(own, 4, p, place(kind)[2])
        terms = [out, at(par, 8, p, kind)]
        if C <= kind < OWN:
            terms.append(at(got, 6, p, kind - C))
        if kind >= OWN:
            i = 1 - (kind - OWN)
            terms += [at(got, 6, p, C + i), at(got, 6, p, B + 1 - i)]

        def body(r, carry):
            rows = pl.ds(pl.multiple_of(r * GROUP, GROUP), GROUP)
            total = terms[0][rows, :].astype(jnp.float32)
            for one in terms[1:]:
                total = total + one[rows, :].astype(jnp.float32)
            total = total.astype(jnp.bfloat16)
            out[rows, :] = total
            if kind >= OWN:
                total = total.astype(jnp.float32)
                total = total * total
                tiles = [total[a : a + 8, b : b + 128] for a in range(0, GROUP, 8) for b in range(0, total.shape[1], 128)]
                sums = [sum(tiles[j::4]) for j in range(4)]
                carry = carry + ((sums[0] + sums[1]) + (sums[2] + sums[3]))
            return carry

        if kind < OWN:
            lax.fori_loop(first, last, body, 0)
        else:
            sq[me] = lax.fori_loop(first, last, body, sq[me])

    for t in range(AHEAD):
        start_load(t)
    barrier = pltpu.get_barrier_semaphore()
    for device in (partner, *beside):
        pl.semaphore_signal(barrier, inc=1, device_id={AXIS: device}, device_id_type=pl.DeviceIdType.MESH)
    pl.semaphore_wait(barrier, 3)
    for r in range(groups(0)):
        for t in range(2):
            give(t, r).start()
    for t in range(2, AHEAD):
        give(t).start()
    sq[me] = jnp.zeros(sq.shape[1:], jnp.float32)

    for r in range(groups(0)):
        for t in range(2):
            if r == 0:
                load(t).wait()
            give(t, r).wait_recv()
            add_up(*steps[t], r, r + 1)
            send(*steps[t], r).start()
    for t, (kind, p) in enumerate(steps):
        if t + AHEAD < len(steps):
            give(t + AHEAD).start()
        if t >= 2:
            load(t).wait()
            give(t).wait_recv()
            if C <= kind < OWN:
                send(kind - C, p).wait_recv()
            if (kind, p) == (OWN + 1, 0):
                for k in each:
                    all_of(B_CAME, k, got[k], 2 * len(places.members[k]))
            if kind >= OWN and p != end:
                send(C + 1 - (kind - OWN), p).wait_recv()
            if p != end or kind < C:
                add_up(kind, p, 0, groups(p))
            if p != end and kind < OWN or kind < C:
                send(kind, p).start()
            if p == end and C <= kind < OWN:
                add_up(kind, p, 0, groups(p))
                for r in range(len(cuts)):
                    send(kind, p, rows=r).start()
            if (kind, p) == (OWN, end):
                for r, (first, size) in enumerate(cuts):
                    for h in (1, 0):
                        send(C + 1 - h, p, rows=r).wait_recv()
                        add_up(OWN + h, p, first, first + size)
        if t + AHEAD < len(steps):
            start_load(t + AHEAD)
        if t == 2 * places.count:
            for q in spots:
                for h in range(2):
                    pltpu.make_async_copy(places.own(m, q, h), at(mm, 2, q, h), shared(M, q)).start()
                    pltpu.make_async_copy(places.own(v, q, h), at(vv, 2, q, h), shared(V, q)).start()
                    pltpu.make_async_copy(places.rows(w, q, me, h), at(ww, 2, q, h), shared(W, q)).start()

    for o in range(1, n):
        remote(sq.at[me], sq.at[me], all_sem.at[TOLD, 0], all_sem.at[HEARD, 0], lax.rem(me + o, n)).start()
    for k in each:
        all_of(SUM_C, k, own[k], 2 * len(places.members[k]))
        all_of(SUM_GIVEN, k, par[k], None)
        for what, buffers in ((M, mm), (V, vv), (W, ww)):
            all_of(what, k, buffers[k], None)
    all_of(HEARD, 0, sq, n - 1)
    total = sq[0]
    for d in range(1, n):
        total = total + sq[d]
    total = jnp.full(factor_ref.shape, jnp.sum(total), jnp.float32)
    factor_ref[...] = jnp.minimum(1.0, 0.5 * lax.rsqrt(total / count + 1e-30))

    def ahead(i, p, h, r=None):
        there = part(places.rows(whole, p, me, h), r)
        return remote(part(at(ww, 2, p, h), r), there, shared(SENT, p), came_sem.at[p, i], beside[i])

    def ahead_came(i, p):
        here = places.rows(whole, p, away(-sign[i], core), 1 - i)
        return remote(here, here, shared(SENT, p), came_sem.at[p, i], beside[i])

    def onward(i, p):
        here = places.rows(whole, p, away(-sign[i], core), 1 - i)
        if p == end:
            return remote(here, last.at[i], extra_send.at[i], pass_sem.at[p, i], beside[i])
        return remote(here, last.at[4 + i] if p == prev else here, shared(SENT, p), pass_sem.at[p, i], beside[i])

    def onward_came(i, p):
        here = places.rows(whole, p, away(2, core), 1 - i)
        return remote(here, here, shared(SENT, p), pass_sem.at[p, i], beside[i])

    def extra(i):
        here = places.rows(whole, end, away(-sign[i], 1 - core), 1 - i)
        return remote(here, last.at[2 + i], extra_send.at[2 + i], extra_recv.at[i], beside[i])

    def across(k, p):
        if k < 2:
            here = places.rows(whole, p, away(-sign[k], core), 1 - k)
        elif k < 4:
            here = places.rows(whole, p, away(2, core), 1 - (k - 2))
        else:
            here = places.rows(whole, p, me, k - 4)
        src = here if k < 4 else at(ww, 2, p, k - 4)
        recv = end_recv.at[k] if p == end and k < 2 else shared(ACROSS_CAME, p)
        return remote(src, here, shared(ACROSS, p), recv, partner)

    def side_came_across(i):
        here = places.rows(whole, end, away(-sign[i], 1 - core), 1 - i)
        return remote(here, here, end_recv.at[i], end_recv.at[i], partner)

    def update(p, h, first, last):
        gs, ms, vs, ws = at(own, 4, p, 3 - h), at(mm, 2, p, h), at(vv, 2, p, h), at(ww, 2, p, h)

        def body(r, carry):
            rows = pl.ds(pl.multiple_of(r * GROUP, GROUP), GROUP)
            grad = gs[rows, :].astype(jnp.float32) * factor_ref[0:1, 0:1]
            ws[rows, :], ms[rows, :], vs[rows, :] = adamw(ws[rows, :].astype(jnp.float32), ms[rows, :], vs[rows, :], grad)
            return carry

        lax.fori_loop(first, last, body, 0)

    for r in range(groups(0)):
        for h in (1, 0):
            update(0, h, r, r + 1)
            ahead(1 - h, 0, h, r).start()
    for p in spots:
        for h in (1, 0):
            if p:
                update(p, h, 0, groups(p))
                ahead(1 - h, p, h).start()
            across(4 + h, p).start()
            pltpu.make_async_copy(at(ww, 2, p, h), places.rows(whole, p, me, h), shared(KEPT, p)).start()
            for k, one in enumerate(places.groups):
                start = 0
                for q, first, size in one:
                    if q == p:
                        src, dst = at(ww, 2, p, h).at[pl.ds(first, size), :], tails[2 * k + h].at[pl.ds(start, size), :]
                        pltpu.make_async_copy(src, dst, shared(HANDED, p)).start()
                    start += size
    for p in spots:
        for i in range(2):
            ahead_came(i, p).wait_recv()
            if p != end:
                onward(i, p).start()
            across(i, p).start()

    @pl.when(second)
    def _():
        for i in range(2):
            onward(i, end).start()
        for i in range(2):
            side_came_across(i).wait_recv()
            extra(i).start()

    for p in spots[:-1]:
        for i in range(2):
            onward_came(i, p).wait_recv()
            if p != prev:
                across(2 + i, p).start()
    for k in each:
        members = len(places.members[k])
        ends = 1 if k == kind_of(end) else 0
        all_of(SENT, k, own[k], 4 * members - 2 * ends)
        all_of(ACROSS, k, par[k], 6 * members - 4 * ends)
        all_of(ACROSS_CAME, k, par[k], 6 * members - 6 * ends)
        all_of(KEPT, k, ww[k], None)
        all_of(HANDED, k, ww[k], None)
    all_of(TOLD, 0, sq, n - 1)

    @pl.when(second)
    def _():
        for i in range(2):
            for copy in (onward(i, end), extra(i)):
                copy.wait()

    @pl.when(jnp.logical_not(second))
    def _():
        for i in range(2):
            side_came_across(i).wait_recv()


def gather_new(terms, weights, m, v, n):
    shapes = [w.shape for w in weights]
    places = Places(n, shapes)
    count = float(sum(w.size for w in weights))
    anywhere, vmem = pl.BlockSpec(memory_space=pl.ANY), pl.BlockSpec(memory_space=pltpu.VMEM)
    out = [pltpu.HBM(s, jnp.bfloat16) for s in shapes]
    out += places.scratch(2, jnp.float32) * 2
    out += [jax.ShapeDtypeStruct((8, 128), jnp.float32)]
    out += [jax.ShapeDtypeStruct(shape, jnp.bfloat16) for shape, _ in places.late for _ in range(2)]
    out += [jax.ShapeDtypeStruct((6, *places.piece[-1]), jnp.bfloat16)]
    dma = pltpu.SemaphoreType.DMA
    half, nk = jnp.bfloat16, len(places.kinds)
    scratch = [
        *places.scratch(4, half), *places.scratch(8, half), *places.scratch(6, half),
        *places.scratch(2, half),
        pltpu.VMEM((n, 8, 128), jnp.float32),
        dma((RING,)), dma((2, places.half[0] // GROUP)), dma((2 * RING,)), dma((places.count, 2)), dma((places.count, 2)),
        dma((15, nk)), dma((4,)), dma((2,)), dma((2,)), dma((2, len(places.cuts()))),
    ]
    got = pl.pallas_call(
        functools.partial(exchange, places, count),
        out_shape=out,
        in_specs=[anywhere] * 12,
        out_specs=[anywhere] * 3 + [vmem] * (2 * nk + 1) + [anywhere] * (2 * len(places.groups) + 1),
        scratch_shapes=scratch,
        compiler_params=pltpu.CompilerParams(collective_id=0, has_side_effects=True, vmem_limit_bytes=46 * 1000 * 1000),
        name="exchange",
    )(*terms, *weights, *m, *v)
    got_m, got_v, rest = got[3 : 3 + nk], got[3 + nk : 3 + 2 * nk], got[4 + 2 * nk :]
    return got[:3], got_m, got_v, rest[:-1], rest[-1]


def params(**more):
    return pltpu.CompilerParams(has_side_effects=False, **more)


def finish(places, tail, *refs):
    nk = len(places.kinds)
    parts, i = [], 0
    for size in (3, nk, nk, 3, 3, 3, nk, 1, 1, 1):
        parts.append(refs[i : i + size])
        i += size
    whole, mm, vv, out, new_m, new_v, slots, (in_sem,), (out_sem,), (put_sem,) = parts
    n = places.n
    chips = n // CORES
    chip = lax.div(lax.axis_index(AXIS), CORES)
    pieces = [(p, h) for p in range(places.count) for h in range(2)]

    def puts(p, h):
        refs = ((mm, new_m), (vv, new_v))
        return [pltpu.make_async_copy(places.at(a, 2, p, h), places.own(b, p, h), put_sem.at[j, places.spot(p)[0]]) for j, (a, b) in enumerate(refs)]

    items = []
    for p, h in pieces:
        for k in range(chips):
            if p in tail and k == (1 if h else chips - 1) or p >= places.end - 1 and k == 2:
                continue
            items += [(p, h, k, c) for c in range(CORES)]
    turn, of_kind = [], [[] for _ in range(nk)]
    for t, (p, *_) in enumerate(items):
        kind, _ = places.spot(p)
        turn.append((kind, len(of_kind[kind])))
        of_kind[kind].append(t)

    def ends(t):
        p, h, k, c = items[t]
        block = lax.rem(chip + k, chips) * CORES + c
        kind, u = turn[t]
        return places.rows(whole, p, block, h), slots[kind].at[u % SLOTS], places.rows(out, p, block, h), (kind, u % SLOTS)

    def read(t):
        src, slot, _, sem = ends(t)
        return pltpu.make_async_copy(src, slot, in_sem.at[sem])

    def write(t):
        _, slot, dst, sem = ends(t)
        return pltpu.make_async_copy(slot, dst, out_sem.at[sem])

    def start_read(t):
        kind, u = turn[t]
        if u >= SLOTS:
            write(of_kind[kind][u - SLOTS]).wait()
        read(t).start()

    for t in range(min(DEPTH, len(items))):
        start_read(t)
    done = 0
    for t in range(len(items)):
        read(t).wait()
        write(t).start()
        if t + DEPTH < len(items):
            start_read(t + DEPTH)
        while done * len(items) < (t + 1) * len(pieces) and done < len(pieces):
            for copy in puts(*pieces[done]):
                copy.start()
            done += 1
    for kind in range(nk):
        for t in of_kind[kind][-SLOTS:]:
            write(t).wait()
    for kind in range(nk):
        for j, one in enumerate((mm, vv)):
            pltpu.make_async_copy(one[kind], one[kind], put_sem.at[j, kind]).wait()


def finish_all(places, tail, whole, mm, vv, m, v):
    anywhere, vmem = pl.BlockSpec(memory_space=pl.ANY), pl.BlockSpec(memory_space=pltpu.VMEM)
    dma = pltpu.SemaphoreType.DMA
    nk = len(places.kinds)
    size = sum(w.size for w in whole)
    mine = sum(one.size for one in m)
    whole = [pltpu.with_memory_space_constraint(w, pltpu.HBM) for w in whole]
    mm, vv = ([pltpu.with_memory_space_constraint(one, pltpu.VMEM) for one in x] for x in (mm, vv))
    return pl.pallas_call(
        functools.partial(finish, places, tail),
        out_shape=[jax.ShapeDtypeStruct(a.shape, a.dtype) for a in (*whole, *m, *v)],
        in_specs=[anywhere] * 3 + [vmem] * (2 * nk),
        out_specs=[anywhere] * 9,
        scratch_shapes=[
            *(pltpu.VMEM((SLOTS, *k), jnp.bfloat16) for k in places.kinds),
            dma((nk, SLOTS)), dma((nk, SLOTS)), dma((2, nk)),
        ],
        compiler_params=params(vmem_limit_bytes=24 * 1024 * 1024),
        cost_estimate=pl.CostEstimate(flops=size * 100, bytes_accessed=size * 4 + mine * 8, transcendentals=0),
        name="finish",
    )(*whole, *mm, *vv)


def place_late(places, spots, *refs):
    k = max(one[0] for one in spots) + 1
    arrays, out, sem = refs[:k], refs[k + 3 : k + 6], refs[k + 6]
    chips = places.n // CORES
    me = lax.axis_index(AXIS)
    core, chip = lax.rem(me, CORES), lax.div(me, CORES)
    jobs = {}
    for number, (a, only, src, (p, first, size), h, away, (relative, which)) in enumerate(spots):
        block = lax.rem(chip + (away + chips), chips) * CORES + (lax.rem(core + which, CORES) if relative else which)
        src = arrays[a].at[src] if isinstance(src, int) else arrays[a].at[pl.ds(src[0], size), :]
        jobs.setdefault(only, []).append(pltpu.make_async_copy(src, places.rows(out, p, block, h, first, size), sem.at[number]))

    def run(copies):
        for copy in copies:
            copy.start()
        for copy in copies:
            copy.wait()

    for only, copies in jobs.items():
        run(copies) if only is None else pl.when(core == only)(functools.partial(run, copies))


def place_all(places, spots, arrays, out):
    anywhere, vmem = pl.BlockSpec(memory_space=pl.ANY), pl.BlockSpec(memory_space=pltpu.VMEM)
    k = len(arrays)
    return pl.pallas_call(
        functools.partial(place_late, places, spots),
        out_shape=[jax.ShapeDtypeStruct(w.shape, w.dtype) for w in out],
        in_specs=[vmem] * k + [anywhere] * 3,
        out_specs=[anywhere] * 3,
        input_output_aliases={k + j: j for j in range(3)},
        scratch_shapes=[pltpu.SemaphoreType.DMA((len(spots),))],
        compiler_params=params(vmem_limit_bytes=16 * 1024 * 1024),
        cost_estimate=pl.CostEstimate(flops=10**7, bytes_accessed=sum(x.size for x in arrays) * 4, transcendentals=0),
        name="place_late",
    )(*arrays, *out)


def solution(mesh):
    n = mesh.shape[AXIS]
    chips = n // CORES

    def step(*arrays):
        terms, weights, m, v = (arrays[i : i + 3] for i in (0, 3, 6, 9))
        places = Places(n, [w.shape for w in weights])
        tail = list(range(places.count))
        whole, mm, vv, late, last = gather_new([t[0] for t in terms], weights, m, v, n)
        groups = range(len(places.groups))
        shift = [[(j, (j // CORES + s) % chips * CORES + j % CORES) for j in range(n)] for s in (1, -1)]
        swap = [(j, j // CORES * CORES + (CORES - 1 - j % CORES)) for j in range(n)]
        came = []
        for k in groups:
            came.append([lax.ppermute(late[2 * k + h], AXIS, shift[h]) for h in range(2)])
        last_swapped = lax.ppermute(last, AXIS, swap)
        *out, m0, m1, m2, v0, v1, v2 = finish_all(places, tail, whole, mm, vv, m, v)
        own, other = (True, 0), (True, 1)

        def spots(k, which, base):
            found = []
            for h in range(2):
                start = 0
                for p, first, size in places.groups[k]:
                    found.append((base + h, None, (start,), (p, first, size), h, -1 if h == 0 else 1, which))
                    start += size
            return found

        end, rows = places.end, places.kinds[-1][0]
        far = lambda a, only, j, p, i, c: (a, only, j + i, (p, 0, rows), 1 - i, 2, (False, c))
        ends = []
        for i in range(2):
            ends += [far(0, 1, 0, end, i, 1), far(0, 1, 2, end, i, 0), far(0, 1, 4, end - 1, i, 1), far(1, 1, 4, end - 1, i, 0)]
            ends += [far(1, 0, 0, end, i, 1), far(1, 0, 2, end, i, 0), far(1, 0, 4, end - 1, i, 1), far(0, 0, 4, end - 1, i, 0)]
        out = place_all(places, ends, [last, last_swapped], out)
        crossed = {}
        for k in groups:
            here, out = lax.optimization_barrier((came[k], out))
            crossed[k] = [lax.ppermute(piece, AXIS, swap) for piece in here]
            out = place_all(places, spots(k, own, 0), here, out)
            if k == 0:
                out = place_all(places, spots(k, other, 0), crossed.pop(k), out)
        work = [one for j, k in enumerate(crossed) for one in spots(k, other, 2 * j)]
        out = place_all(places, work, [piece for one in crossed.values() for piece in one], out)
        return (*out, m0, m1, m2, v0, v1, v2)

    all_of, cut = P(None, None, None), P(None, AXIS, None)
    return jax.shard_map(
        step,
        mesh=mesh,
        in_specs=(P(("rep", AXIS), None, None, None),) * 3 + (all_of,) * 3 + (cut,) * 6,
        out_specs=(P("rep", None, None),) * 3 + (P("rep", AXIS, None),) * 6,
        check_vma=False,
    )
```

```python
import functools

import jax
import jax.numpy as jnp
from jax import lax
from jax.experimental import pallas as pl
from jax.experimental.pallas import tpu as pltpu
from jax.sharding import PartitionSpec as P


AXIS = "dp"
CORES = 2
AHEAD = 4
GROUP = 16
RING = 8
SLOTS, DEPTH = 16, 8
A, B, C, OWN = 0, 2, 4, 6


def adamw(w, m, v, g):
    m = 0.9 * m + 0.1 * g
    v = 0.95 * v + 0.05 * g * g
    step = m * lax.rsqrt(v + 1e-8) + 0.1 * w
    return (w - 0.02 * step).astype(jnp.bfloat16), m, v


class Places:
    def __init__(self, n, shapes):
        self.n = n
        self.layers = shapes[0][0]
        self.half = [rows // n // 2 for _, rows, _ in shapes]
        self.piece = [(h, cols) for h, (_, _, cols) in zip(self.half, shapes)]
        self.count = len(shapes) * self.layers
        self.kinds = sorted(set(self.piece), key=self.piece.index)
        self.members = [[p for p in range(self.count) if self.piece[p // self.layers] == k] for k in self.kinds]

        self.end = self.count - 1
        whole = [[(p, 0, k[0]) for p in m] for m, k in zip(self.members, self.kinds)]
        rows = self.kinds[-1][0]
        cut = (rows // GROUP + 1) // 2 * GROUP
        self.groups = [*whole[:-1], whole[-1][:-1] + [(self.end, 0, cut)], [(self.end, cut, rows - cut)]]
        self.late = [((sum(r for _, _, r in one), self.piece[one[0][0] // self.layers][1]), one) for one in self.groups]

    def cuts(self):
        n = self.kinds[-1][0] // GROUP
        size = -(-n // 8)
        return [(a, min(size, n - a)) for a in range(0, n, size)]

    def scratch(self, slots, dtype):
        return [pltpu.VMEM((len(m) * slots, *k), dtype) for m, k in zip(self.members, self.kinds)]

    def spot(self, p):
        kind = self.kinds.index(self.piece[p // self.layers])
        return kind, self.members[kind].index(p)

    def at(self, buffers, slots, p, slot):
        kind, j = self.spot(p)
        return buffers[kind].at[j * slots + slot]

    def rows(self, refs, p, block, half, first=0, size=None):
        w = p // self.layers
        start = pl.multiple_of((block * 2 + half) * self.half[w] + first, GROUP)
        return refs[w].at[p % self.layers, pl.ds(start, self.half[w] if size is None else size), :]

    def own(self, refs, p, half):
        w = p // self.layers
        return refs[w].at[p % self.layers, pl.ds(half * self.half[w], self.half[w]), :]


def exchange(places, count, *refs):
    nk = len(places.kinds)
    names = (3, 3, 3, 3, 3, nk, nk, 1, 2 * len(places.groups) + 1, nk, nk, nk, nk, *(1,) * 11)
    parts, i = [], 0
    for size in names:
        parts.append(refs[i : i + size])
        i += size
    g, w, m, v, whole, mm, vv, (factor_ref,), (*tails, last) = parts[:9]
    own, par, got, ww = parts[9:13]
    (sq,), (own_sem,), (first_sem,), (par_recv,), (came_sem,), (pass_sem,), (all_sem,), (extra_send,), (extra_recv,), (end_recv,), (cut_sem,) = parts[13:]

    n, at, end = places.n, places.at, places.end
    prev = end - 1
    chips = n // CORES
    me = lax.axis_index(AXIS)
    core, chip = lax.rem(me, CORES), lax.div(me, CORES)
    away = lambda k, core: lax.rem(chip + (k + chips), chips) * CORES + core
    partner = away(0, 1 - core)
    sign = (1, -1)
    beside = [away(s, core) for s in sign]
    second = core == CORES - 1
    kind_of = lambda p: places.spot(p)[0]
    each = range(nk)

    def remote(src, dst, send, recv, device):
        return pltpu.make_async_remote_copy(
            src_ref=src, dst_ref=dst, send_sem=send, recv_sem=recv, device_id={AXIS: device}, device_id_type=pl.DeviceIdType.MESH
        )

    SUM_GIVEN, SUM_A, SUM_B, SUM_C, B_CAME, M, V, W, SENT, ACROSS, ACROSS_CAME, KEPT, HANDED, TOLD, HEARD = range(15)
    shared = lambda what, p: all_sem.at[what, kind_of(p)]

    def all_of(what, kind, ref, size):
        sem, ref = all_sem.at[what, kind], ref if size is None else ref.at[pl.ds(0, size)]
        remote(ref, ref, sem, sem, partner).wait_recv()

    def place(kind):
        i = kind % 2
        if kind < B:
            return 2, 1 - i, i
        if kind < C:
            return sign[i], i, 2 + i
        if kind < OWN:
            return sign[i], 1 - i, i
        return 0, i, 3 - i

    spots = range(places.count)
    steps = [(k + i, p) for k in (A, B, C) for p in spots for i in range(2)] + [(OWN + h, p) for p in spots for h in (1, 0)]
    groups = lambda p: places.half[p // places.layers] // GROUP
    cuts = places.cuts()
    part = lambda ref, r: ref if r is None else ref.at[pl.ds(r * GROUP, GROUP), :]

    def load(t):
        kind, p = steps[t]
        to, half, slot = place(kind)
        return pltpu.make_async_copy(places.rows(g, p, away(to, core), half), at(own, 4, p, slot), own_sem.at[t % RING])

    def give(t, r=None):
        kind, p = steps[t]
        to, half, _ = place(kind)
        recv = par_recv.at[t % (2 * RING)] if r is None else first_sem.at[t, r]
        src, dst = part(places.rows(g, p, away(to, 1 - core), half), r), part(at(par, 8, p, kind), r)
        return remote(src, dst, shared(SUM_GIVEN, p), recv, partner)

    def send(kind, p, r=None, rows=None):
        what, i = (SUM_A, SUM_B, SUM_C)[kind // 2], kind % 2
        recv = (came_sem.at[p, i], shared(B_CAME, p), pass_sem.at[p, i])[kind // 2]
        src, dst = part(at(own, 4, p, place(kind)[2]), r), part(at(got, 6, p, kind), r)
        if rows is not None:
            first, size = cuts[rows]
            src, dst = (ref.at[pl.ds(first * GROUP, size * GROUP), :] for ref in (src, dst))
            recv = cut_sem.at[i, rows]
        return remote(src, dst, shared(what, p), recv, beside[i])

    def start_load(t):
        if steps[t] in ((C, 0), (OWN + 1, 0)):
            for k in each:
                all_of(SUM_A if steps[t][0] < OWN else SUM_B, k, own[k], 2 * len(places.members[k]))
        load(t).start()

    def add_up(kind, p, first, last):
        out = at(own, 4, p, place(kind)[2])
        terms = [out, at(par, 8, p, kind)]
        if C <= kind < OWN:
            terms.append(at(got, 6, p, kind - C))
        if kind >= OWN:
            i = 1 - (kind - OWN)
            terms += [at(got, 6, p, C + i), at(got, 6, p, B + 1 - i)]

        def body(r, carry):
            rows = pl.ds(pl.multiple_of(r * GROUP, GROUP), GROUP)
            total = terms[0][rows, :].astype(jnp.float32)
            for one in terms[1:]:
                total = total + one[rows, :].astype(jnp.float32)
            total = total.astype(jnp.bfloat16)
            out[rows, :] = total
            if kind >= OWN:
                total = total.astype(jnp.float32)
                total = total * total
                tiles = [total[a : a + 8, b : b + 128] for a in range(0, GROUP, 8) for b in range(0, total.shape[1], 128)]
                sums = [sum(tiles[j::4]) for j in range(4)]
                carry = carry + ((sums[0] + sums[1]) + (sums[2] + sums[3]))
            return carry

        if kind < OWN:
            lax.fori_loop(first, last, body, 0)
        else:
            sq[me] = lax.fori_loop(first, last, body, sq[me])

    barrier = pltpu.get_barrier_semaphore()
    for device in (*beside, partner):
        pl.semaphore_signal(barrier, inc=1, device_id={AXIS: device}, device_id_type=pl.DeviceIdType.MESH)
    for t in range(2):
        start_load(t)
    sq[me] = jnp.zeros(sq.shape[1:], jnp.float32)
    pl.semaphore_wait(barrier, 3)
    for r in range(groups(0)):
        for t in range(2):
            give(t, r).start()
    for t in range(2, AHEAD):
        give(t).start()
        start_load(t)

    for r in range(groups(0)):
        for t in range(2):
            if r == 0:
                load(t).wait()
            give(t, r).wait_recv()
            add_up(*steps[t], r, r + 1)
            send(*steps[t], r).start()
    for t, (kind, p) in enumerate(steps):
        if t + AHEAD < len(steps):
            give(t + AHEAD).start()
        if t >= 2:
            load(t).wait()
            give(t).wait_recv()
            if C <= kind < OWN:
                send(kind - C, p).wait_recv()
            if (kind, p) == (OWN + 1, 0):
                for k in each:
                    all_of(B_CAME, k, got[k], 2 * len(places.members[k]))
            if kind >= OWN and p != end:
                send(C + 1 - (kind - OWN), p).wait_recv()
            if p != end or kind < C:
                add_up(kind, p, 0, groups(p))
            if p != end and kind < OWN or kind < C:
                send(kind, p).start()
            if p == end and C <= kind < OWN:
                add_up(kind, p, 0, groups(p))
                for r in range(len(cuts)):
                    send(kind, p, rows=r).start()
            if (kind, p) == (OWN, end):
                for r, (first, size) in enumerate(cuts):
                    for h in (1, 0):
                        send(C + 1 - h, p, rows=r).wait_recv()
                        add_up(OWN + h, p, first, first + size)
        if t + AHEAD < len(steps):
            start_load(t + AHEAD)
        if t == 2 * places.count:
            for q in spots:
                for h in range(2):
                    pltpu.make_async_copy(places.own(m, q, h), at(mm, 2, q, h), shared(M, q)).start()
                    pltpu.make_async_copy(places.own(v, q, h), at(vv, 2, q, h), shared(V, q)).start()
                    pltpu.make_async_copy(places.rows(w, q, me, h), at(ww, 2, q, h), shared(W, q)).start()

    for o in sorted(range(1, n), key=lambda o: -min(o, n - o)):
        remote(sq.at[me], sq.at[me], all_sem.at[TOLD, 0], all_sem.at[HEARD, 0], lax.rem(me + o, n)).start()
    for k in each:
        for what, buffers in ((M, mm), (V, vv), (W, ww)):
            all_of(what, k, buffers[k], None)
    all_of(HEARD, 0, sq, n - 1)
    total = sq[0]
    for d in range(1, n):
        total = total + sq[d]
    total = jnp.full(factor_ref.shape, jnp.sum(total), jnp.float32)
    factor_ref[...] = jnp.minimum(1.0, 0.5 * lax.rsqrt(total / count + 1e-30))

    def ahead(i, p, h, r=None):
        there = part(places.rows(whole, p, me, h), r)
        return remote(part(at(ww, 2, p, h), r), there, shared(SENT, p), came_sem.at[p, i], beside[i])

    def ahead_came(i, p):
        here = places.rows(whole, p, away(-sign[i], core), 1 - i)
        return remote(here, here, shared(SENT, p), came_sem.at[p, i], beside[i])

    def onward(i, p):
        here = places.rows(whole, p, away(-sign[i], core), 1 - i)
        if p == end:
            return remote(here, last.at[i], extra_send.at[i], pass_sem.at[p, i], beside[i])
        return remote(here, last.at[4 + i] if p == prev else here, shared(SENT, p), pass_sem.at[p, i], beside[i])

    def onward_came(i, p):
        here = places.rows(whole, p, away(2, core), 1 - i)
        return remote(here, here, shared(SENT, p), pass_sem.at[p, i], beside[i])

    def extra(i):
        here = places.rows(whole, end, away(-sign[i], 1 - core), 1 - i)
        return remote(here, last.at[2 + i], extra_send.at[2 + i], extra_recv.at[i], beside[i])

    def across(k, p):
        if k < 2:
            here = places.rows(whole, p, away(-sign[k], core), 1 - k)
        elif k < 4:
            here = places.rows(whole, p, away(2, core), 1 - (k - 2))
        else:
            here = places.rows(whole, p, me, k - 4)
        src = here if k < 4 else at(ww, 2, p, k - 4)
        recv = end_recv.at[k] if p == end and k < 2 else shared(ACROSS_CAME, p)
        return remote(src, here, shared(ACROSS, p), recv, partner)

    def side_came_across(i):
        here = places.rows(whole, end, away(-sign[i], 1 - core), 1 - i)
        return remote(here, here, end_recv.at[i], end_recv.at[i], partner)

    def update(p, h, first, last):
        gs, ms, vs, ws = at(own, 4, p, 3 - h), at(mm, 2, p, h), at(vv, 2, p, h), at(ww, 2, p, h)

        def body(r, carry):
            rows = pl.ds(pl.multiple_of(r * GROUP, GROUP), GROUP)
            grad = gs[rows, :].astype(jnp.float32) * factor_ref[0:1, 0:1]
            ws[rows, :], ms[rows, :], vs[rows, :] = adamw(ws[rows, :].astype(jnp.float32), ms[rows, :], vs[rows, :], grad)
            return carry

        lax.fori_loop(first, last, body, 0)

    for r in range(groups(0)):
        for h in (1, 0):
            update(0, h, r, r + 1)
            ahead(1 - h, 0, h, r).start()
    for p in spots:
        for h in (1, 0):
            if p:
                update(p, h, 0, groups(p))
                ahead(1 - h, p, h).start()
            across(4 + h, p).start()
            pltpu.make_async_copy(at(ww, 2, p, h), places.rows(whole, p, me, h), shared(KEPT, p)).start()
            for k, one in enumerate(places.groups):
                start = 0
                for q, first, size in one:
                    if q == p:
                        src, dst = at(ww, 2, p, h).at[pl.ds(first, size), :], tails[2 * k + h].at[pl.ds(start, size), :]
                        pltpu.make_async_copy(src, dst, shared(HANDED, p)).start()
                    start += size
    for p in spots:
        for i in range(2):
            ahead_came(i, p).wait_recv()
            if p != end:
                onward(i, p).start()
            across(i, p).start()

    @pl.when(second)
    def _():
        for i in range(2):
            onward(i, end).start()
        for i in range(2):
            side_came_across(i).wait_recv()
            extra(i).start()

    for p in spots[:-1]:
        for i in range(2):
            onward_came(i, p).wait_recv()
            if p != prev:
                across(2 + i, p).start()
    for k in each:
        members = len(places.members[k])
        ends = 1 if k == kind_of(end) else 0
        all_of(SUM_C, k, own[k], 2 * members)
        all_of(SUM_GIVEN, k, par[k], None)
        all_of(SENT, k, own[k], 4 * members - 2 * ends)
        all_of(ACROSS, k, par[k], 6 * members - 4 * ends)
        all_of(ACROSS_CAME, k, par[k], 6 * members - 6 * ends)
        all_of(KEPT, k, ww[k], None)
        all_of(HANDED, k, ww[k], None)
    all_of(TOLD, 0, sq, n - 1)

    @pl.when(second)
    def _():
        for i in range(2):
            for copy in (onward(i, end), extra(i)):
                copy.wait()

    @pl.when(jnp.logical_not(second))
    def _():
        for i in range(2):
            side_came_across(i).wait_recv()


def gather_new(terms, weights, m, v, n):
    shapes = [w.shape for w in weights]
    places = Places(n, shapes)
    count = float(sum(w.size for w in weights))
    anywhere, vmem = pl.BlockSpec(memory_space=pl.ANY), pl.BlockSpec(memory_space=pltpu.VMEM)
    out = [pltpu.HBM(s, jnp.bfloat16) for s in shapes]
    out += places.scratch(2, jnp.float32) * 2
    out += [jax.ShapeDtypeStruct((8, 128), jnp.float32)]
    out += [jax.ShapeDtypeStruct(shape, jnp.bfloat16) for shape, _ in places.late for _ in range(2)]
    out += [jax.ShapeDtypeStruct((6, *places.piece[-1]), jnp.bfloat16)]
    dma = pltpu.SemaphoreType.DMA
    half, nk = jnp.bfloat16, len(places.kinds)
    scratch = [
        *places.scratch(4, half), *places.scratch(8, half), *places.scratch(6, half),
        *places.scratch(2, half),
        pltpu.VMEM((n, 8, 128), jnp.float32),
        dma((RING,)), dma((2, places.half[0] // GROUP)), dma((2 * RING,)), dma((places.count, 2)), dma((places.count, 2)),
        dma((15, nk)), dma((4,)), dma((2,)), dma((2,)), dma((2, len(places.cuts()))),
    ]
    got = pl.pallas_call(
        functools.partial(exchange, places, count),
        out_shape=out,
        in_specs=[anywhere] * 12,
        out_specs=[anywhere] * 3 + [vmem] * (2 * nk + 1) + [anywhere] * (2 * len(places.groups) + 1),
        scratch_shapes=scratch,
        compiler_params=pltpu.CompilerParams(collective_id=0, has_side_effects=True, vmem_limit_bytes=46 * 1000 * 1000),
        name="exchange",
    )(*terms, *weights, *m, *v)
    got_m, got_v, rest = got[3 : 3 + nk], got[3 + nk : 3 + 2 * nk], got[4 + 2 * nk :]
    return got[:3], got_m, got_v, rest[:-1], rest[-1]


def params(**more):
    return pltpu.CompilerParams(has_side_effects=False, **more)


def finish(places, tail, *refs):
    nk = len(places.kinds)
    parts, i = [], 0
    for size in (3, nk, nk, 3, 3, 3, nk, 1, 1, 1):
        parts.append(refs[i : i + size])
        i += size
    whole, mm, vv, out, new_m, new_v, slots, (in_sem,), (out_sem,), (put_sem,) = parts
    n = places.n
    chips = n // CORES
    chip = lax.div(lax.axis_index(AXIS), CORES)
    pieces = [(p, h) for p in range(places.count) for h in range(2)]

    def puts(p, h):
        refs = ((mm, new_m), (vv, new_v))
        return [pltpu.make_async_copy(places.at(a, 2, p, h), places.own(b, p, h), put_sem.at[j, places.spot(p)[0]]) for j, (a, b) in enumerate(refs)]

    items = []
    for p, h in pieces:
        for k in range(chips):
            if p in tail and k == (1 if h else chips - 1) or p >= places.end - 1 and k == 2:
                continue
            items += [(p, h, k, c) for c in range(CORES)]
    turn, of_kind = [], [[] for _ in range(nk)]
    for t, (p, *_) in enumerate(items):
        kind, _ = places.spot(p)
        turn.append((kind, len(of_kind[kind])))
        of_kind[kind].append(t)

    def ends(t):
        p, h, k, c = items[t]
        block = lax.rem(chip + k, chips) * CORES + c
        kind, u = turn[t]
        return places.rows(whole, p, block, h), slots[kind].at[u % SLOTS], places.rows(out, p, block, h), (kind, u % SLOTS)

    def read(t):
        src, slot, _, sem = ends(t)
        return pltpu.make_async_copy(src, slot, in_sem.at[sem])

    def write(t):
        _, slot, dst, sem = ends(t)
        return pltpu.make_async_copy(slot, dst, out_sem.at[sem])

    def start_read(t):
        kind, u = turn[t]
        if u >= SLOTS:
            write(of_kind[kind][u - SLOTS]).wait()
        read(t).start()

    for t in range(min(DEPTH, len(items))):
        start_read(t)
    done = 0
    for t in range(len(items)):
        read(t).wait()
        write(t).start()
        if t + DEPTH < len(items):
            start_read(t + DEPTH)
        while done * len(items) < (t + 1) * len(pieces) and done < len(pieces):
            for copy in puts(*pieces[done]):
                copy.start()
            done += 1
    for kind in range(nk):
        for t in of_kind[kind][-SLOTS:]:
            write(t).wait()
    for kind in range(nk):
        for j, one in enumerate((mm, vv)):
            pltpu.make_async_copy(one[kind], one[kind], put_sem.at[j, kind]).wait()


def finish_all(places, tail, whole, mm, vv, m, v):
    anywhere, vmem = pl.BlockSpec(memory_space=pl.ANY), pl.BlockSpec(memory_space=pltpu.VMEM)
    dma = pltpu.SemaphoreType.DMA
    nk = len(places.kinds)
    size = sum(w.size for w in whole)
    mine = sum(one.size for one in m)
    whole = [pltpu.with_memory_space_constraint(w, pltpu.HBM) for w in whole]
    mm, vv = ([pltpu.with_memory_space_constraint(one, pltpu.VMEM) for one in x] for x in (mm, vv))
    return pl.pallas_call(
        functools.partial(finish, places, tail),
        out_shape=[jax.ShapeDtypeStruct(a.shape, a.dtype) for a in (*whole, *m, *v)],
        in_specs=[anywhere] * 3 + [vmem] * (2 * nk),
        out_specs=[anywhere] * 9,
        scratch_shapes=[
            *(pltpu.VMEM((SLOTS, *k), jnp.bfloat16) for k in places.kinds),
            dma((nk, SLOTS)), dma((nk, SLOTS)), dma((2, nk)),
        ],
        compiler_params=params(vmem_limit_bytes=24 * 1024 * 1024),
        cost_estimate=pl.CostEstimate(flops=size * 100, bytes_accessed=size * 4 + mine * 8, transcendentals=0),
        name="finish",
    )(*whole, *mm, *vv)


def place_late(places, spots, *refs):
    k = max(one[0] for one in spots) + 1
    arrays, out, sem = refs[:k], refs[k + 3 : k + 6], refs[k + 6]
    chips = places.n // CORES
    me = lax.axis_index(AXIS)
    core, chip = lax.rem(me, CORES), lax.div(me, CORES)
    jobs = {}
    for number, (a, only, src, (p, first, size), h, away, (relative, which)) in enumerate(spots):
        block = lax.rem(chip + (away + chips), chips) * CORES + (lax.rem(core + which, CORES) if relative else which)
        src = arrays[a].at[src] if isinstance(src, int) else arrays[a].at[pl.ds(src[0], size), :]
        jobs.setdefault(only, []).append(pltpu.make_async_copy(src, places.rows(out, p, block, h, first, size), sem.at[number]))

    def run(copies):
        for copy in copies:
            copy.start()
        for copy in copies:
            copy.wait()

    for only, copies in jobs.items():
        run(copies) if only is None else pl.when(core == only)(functools.partial(run, copies))


def place_all(places, spots, arrays, out):
    anywhere, vmem = pl.BlockSpec(memory_space=pl.ANY), pl.BlockSpec(memory_space=pltpu.VMEM)
    k = len(arrays)
    return pl.pallas_call(
        functools.partial(place_late, places, spots),
        out_shape=[jax.ShapeDtypeStruct(w.shape, w.dtype) for w in out],
        in_specs=[vmem] * k + [anywhere] * 3,
        out_specs=[anywhere] * 3,
        input_output_aliases={k + j: j for j in range(3)},
        scratch_shapes=[pltpu.SemaphoreType.DMA((len(spots),))],
        compiler_params=params(vmem_limit_bytes=16 * 1024 * 1024),
        cost_estimate=pl.CostEstimate(flops=10**7, bytes_accessed=sum(x.size for x in arrays) * 4, transcendentals=0),
        name="place_late",
    )(*arrays, *out)


def solution(mesh):
    n = mesh.shape[AXIS]
    chips = n // CORES

    def step(*arrays):
        terms, weights, m, v = (arrays[i : i + 3] for i in (0, 3, 6, 9))
        places = Places(n, [w.shape for w in weights])
        tail = list(range(places.count))
        whole, mm, vv, late, last = gather_new([t[0] for t in terms], weights, m, v, n)
        groups = range(len(places.groups))
        shift = [[(j, (j // CORES + s) % chips * CORES + j % CORES) for j in range(n)] for s in (1, -1)]
        swap = [(j, j // CORES * CORES + (CORES - 1 - j % CORES)) for j in range(n)]
        came = []
        for k in groups:
            came.append([lax.ppermute(late[2 * k + h], AXIS, shift[h]) for h in range(2)])
        last_swapped = lax.ppermute(last, AXIS, swap)
        *out, m0, m1, m2, v0, v1, v2 = finish_all(places, tail, whole, mm, vv, m, v)
        own, other = (True, 0), (True, 1)

        def spots(k, which, base):
            found = []
            for h in range(2):
                start = 0
                for p, first, size in places.groups[k]:
                    found.append((base + h, None, (start,), (p, first, size), h, -1 if h == 0 else 1, which))
                    start += size
            return found

        end, rows = places.end, places.kinds[-1][0]
        far = lambda a, only, j, p, i, c: (a, only, j + i, (p, 0, rows), 1 - i, 2, (False, c))
        ends = []
        for i in range(2):
            ends += [far(0, 1, 0, end, i, 1), far(0, 1, 2, end, i, 0), far(0, 1, 4, end - 1, i, 1), far(1, 1, 4, end - 1, i, 0)]
            ends += [far(1, 0, 0, end, i, 1), far(1, 0, 2, end, i, 0), far(1, 0, 4, end - 1, i, 1), far(0, 0, 4, end - 1, i, 0)]
        out = place_all(places, ends, [last, last_swapped], out)
        crossed = {}
        for k in groups:
            here, out = lax.optimization_barrier((came[k], out))
            crossed[k] = [lax.ppermute(piece, AXIS, swap) for piece in here]
            out = place_all(places, spots(k, own, 0), here, out)
            if k == 0:
                out = place_all(places, spots(k, other, 0), crossed.pop(k), out)
        work = [one for j, k in enumerate(crossed) for one in spots(k, other, 2 * j)]
        out = place_all(places, work, [piece for one in crossed.values() for piece in one], out)
        return (*out, m0, m1, m2, v0, v1, v2)

    all_of, cut = P(None, None, None), P(None, AXIS, None)
    return jax.shard_map(
        step,
        mesh=mesh,
        in_specs=(P(("rep", AXIS), None, None, None),) * 3 + (all_of,) * 3 + (cut,) * 6,
        out_specs=(P("rep", None, None),) * 3 + (P("rep", AXIS, None),) * 6,
        check_vma=False,
    )
```
